128 devices in a mesh: rows: 8 (over y, core), cols: 16 (over z, x).
Axes of the slice: x: 4, y: 4, z: 4, core: 2. Of those that a mesh axis runs over, the one named last changes fastest.
Arguments:
- image: bfloat16 [256, 1024, 128], P('rows', 'cols'), may hold values from -6 to 6
- routes: int32 [32, 128, 4], P('rows', 'cols'), may hold values from 0 to 4095, as said below
- norm_gain: float32 [128], replicated, may hold values from 0.1 to 1.9
- qkv_weight: bfloat16 [128, 384], replicated, may hold values from -25.455844 to 25.455844
- lce_weight: float32 [5, 5, 128], replicated, may hold values from -1.25 to 1.25
- out_weight: bfloat16 [128, 128], replicated, may hold values from -0.5 to 0.5
- mlp_gain: float32 [128], replicated, may hold values from 0.1 to 1.9
- up_weight: bfloat16 [128, 384], replicated, may hold values from -0.5 to 0.5
- down_weight: bfloat16 [384, 128], replicated, may hold values from -0.3125 to 0.3125
Outputs:
- refined: bfloat16 [256, 1024, 128], P('rows', 'cols')
The draws below stay inside these ranges and needn't reach their ends.
Inputs may be any that keep to these rules, and one draw needn't show every extreme that they name: Each region names 4 different regions. Of the routes of the regions of one device, at most 2 lead to the regions of any one device, and in every draw some device receives exactly 2 from every device.
All inputs are finite; a program needn't handle non-finite values.
Results may differ from the reference program's by a relative error of at most 0.0038.
The reference program's roundings to bfloat16 on the way (of `normed`, `projected`, `weights`, `combined`, `residual`, `second` and `hidden`) count: a program that leaves them out, or rounds other values in their place, can miss the bound.
Values may be sent and summed in bfloat16 or wider, within the bound.
A program may use at most 128 MiB of HBM per device.

```python
import math
import jax
import jax.numpy as jnp
from jax import lax

C = 128
HEADS = 4
FFN = 384
RS = 8
TOPK = 4
KSIZE = 5
RR = 4
RC = 8
CAP = 2
NRR = 32
NRC = 128
GRID_H = 256
GRID_W = 1024


def draw_routes(key, part):
    row_devices = NRR // RR
    col_devices = NRC // RC
    devices = row_devices * col_devices
    region_count = RR * RC
    pair_count = region_count * TOPK
    slot_count = devices * CAP
    base_key = jax.random.fold_in(key, 7)
    hot_key, local_key, jitter_key, sender_keys = jax.random.split(base_key, 4)
    hot_dev = jax.random.randint(hot_key, (), 0, devices)
    hot_local = jax.random.randint(local_key, (devices,), 0, region_count)
    owners = jnp.arange(slot_count, dtype=jnp.int32) // CAP

    def one_sender(sender_key):
        perm_key, order_key = jax.random.split(sender_key)
        ranking = jax.random.permutation(perm_key, slot_count).astype(jnp.int32)
        ranking = ranking - slot_count * (owners == hot_dev).astype(jnp.int32)
        ordered = jnp.argsort(ranking, stable=True)
        chosen = owners[ordered[:pair_count]]
        return chosen[jax.random.permutation(order_key, pair_count)]
    destinations = jax.vmap(one_sender)(jax.random.split(sender_keys, devices))
    destinations = destinations.reshape(devices, region_count, TOPK)
    jitter = jax.random.randint(jitter_key, (devices, region_count, 1), 0, 2)
    picks = jnp.arange(TOPK, dtype=jnp.int32)[None, None, :]
    local_index = (hot_local[destinations] + jitter + picks) % region_count
    region_row = destinations // col_devices * RR + local_index // RC
    region_col = destinations % col_devices * RC + local_index % RC
    global_ids = (region_row * NRC + region_col).astype(jnp.int32)
    shaped = global_ids.reshape(row_devices, col_devices, RR, RC, TOPK)
    return shaped.transpose(0, 2, 1, 3, 4).reshape(NRR, NRC, TOPK)


def draw_qkv_weight(key, part):
    first_key = jax.random.fold_in(jax.random.fold_in(key, 11), 0)
    base_draw = jax.random.truncated_normal(first_key, -3.0, 3.0, (C, 3 * C), jnp.float32) * (1.0 / math.sqrt(C))
    return base_draw.astype(jnp.bfloat16)


def block_scale(own_key, extent, pieces, least, largest):
    gain, own = 1.0, jax.random.fold_in(own_key, 6)
    for axis_at, blocks in pieces:
        heights = jnp.exp(jax.random.uniform(jax.random.fold_in(own, axis_at), (blocks,), jnp.float32, least / len(pieces), largest / len(pieces)))
        gain = gain * jnp.repeat(heights, extent[axis_at] // blocks).reshape([-1 if axis == axis_at else 1 for axis in range(len(extent))])
    return gain


def noise(key, extent, width, most, pieces=(), kind=jnp.bfloat16):
    values = jax.random.normal(key, extent, jnp.float32) * width
    if len(pieces) > 0:
        values = block_scale(key, extent, pieces, -0.22, 0.18) * values
    return jnp.clip(values, min=-most, max=most).astype(kind)


def setup_inputs(seed: int = 0) -> dict:
    key_list = jax.random.split(jax.random.key(seed), 10)
    return {
        "image": noise(key_list[0], (GRID_H, GRID_W, C), 1.0, 6.0, ((0, 8), (1, 16))),
        "routes": draw_routes(jax.random.fold_in(key_list[9], 71), 0),
        "norm_gain": jnp.clip(1.0 + 0.18 * jax.random.normal(key_list[2], (C,), jnp.float32), 0.1, 1.9),
        "qkv_weight": draw_qkv_weight(jax.random.fold_in(key_list[9], 71), 0),
        "lce_weight": noise(key_list[4], (KSIZE, KSIZE, C), (KSIZE * KSIZE) ** -0.5, 1.25, (), jnp.float32),
        "out_weight": noise(key_list[5], (C, C), C ** -0.5, 0.5),
        "mlp_gain": jnp.clip(1.0 + 0.18 * jax.random.normal(key_list[6], (C,), jnp.float32), 0.1, 1.9),
        "up_weight": noise(key_list[7], (C, FFN), C ** -0.5, 0.5),
        "down_weight": noise(key_list[8], (FFN, C), FFN ** -0.5, 0.3125),
    }


EPSILON = 1e-06

def layer_norm(values, norm_scale):
    floats = values.astype(jnp.float32)
    centered = floats - lax.optimization_barrier(jnp.mean(floats, axis=-1, keepdims=True))
    spread = lax.optimization_barrier(jnp.mean(centered * centered, axis=-1, keepdims=True))
    return centered * lax.rsqrt(spread + EPSILON) * norm_scale

def to_regions(grid_field, region_side):
    height, grid_width, channels = grid_field.shape
    shaped = grid_field.reshape(height // region_side, region_side, grid_width // region_side, region_side, channels)
    return shaped.transpose(0, 2, 1, 3, 4).reshape(-1, region_side * region_side, channels)

def from_regions(blocks, region_side, height, grid_width):
    channels = blocks.shape[-1]
    shaped = blocks.reshape(height // region_side, grid_width // region_side, region_side, region_side, channels)
    return shaped.transpose(0, 2, 1, 3, 4).reshape(height, grid_width, channels)

def region_attention(queries, keyvals, head_count):
    group_count, length, channels = queries.shape
    head_size = channels // head_count
    q_heads = queries.astype(jnp.float32).reshape(group_count, length, head_count, head_size)
    k_heads = keyvals[..., :channels].astype(jnp.float32).reshape(group_count, -1, head_count, head_size)
    v_heads = keyvals[..., channels:].astype(jnp.float32).reshape(group_count, -1, head_count, head_size)
    scores = jnp.einsum('gqhd,gkhd->ghqk', q_heads, k_heads) * head_size ** (-0.5)
    row_max = lax.optimization_barrier(jnp.max(scores, axis=-1, keepdims=True))
    expons = jnp.exp(scores - row_max)
    weights = (expons / lax.optimization_barrier(jnp.sum(expons, axis=-1, keepdims=True))).astype(jnp.bfloat16)
    blended = jnp.einsum('ghqk,gkhd->gqhd', weights.astype(jnp.float32), v_heads)
    return blended.reshape(group_count, length, channels)

def local_context(padded, kernel, height, grid_width):
    kernel_size = kernel.shape[0]
    summed = jnp.zeros((height, grid_width, padded.shape[-1]), jnp.float32)
    for offset_row in range(kernel_size):
        for offset_col in range(kernel_size):
            window = padded[offset_row:offset_row + height, offset_col:offset_col + grid_width].astype(jnp.float32)
            summed = summed + window * kernel[offset_row, offset_col].astype(jnp.float32)
    return summed

def reference(image, routes, norm_gain, qkv_weight, lce_weight, out_weight, mlp_gain, up_weight, down_weight):
    height, grid_width, channels = image.shape
    normed = layer_norm(image, norm_gain).astype(jnp.bfloat16)
    projected = jnp.dot(normed.reshape(-1, channels), qkv_weight, preferred_element_type=jnp.float32)
    projected = projected.astype(jnp.bfloat16).reshape(height, grid_width, 3 * channels)
    queries = to_regions(projected[..., :channels], RS)
    keyvals = to_regions(projected[..., channels:], RS)
    values = projected[..., 2 * channels:]
    margin = (lce_weight.shape[0] - 1) // 2
    padded = jnp.pad(values, ((margin, margin), (margin, margin), (0, 0)))
    context = local_context(padded, lce_weight, height, grid_width)
    row_queries = queries.reshape(NRR, NRC, RS * RS, channels)

    def attend(inputs):
        row_block, row_routes = inputs
        chosen = keyvals[row_routes.reshape(-1)].reshape(NRC, TOPK * RS * RS, 2 * channels)
        return region_attention(row_block, chosen, HEADS)
    blended = lax.map(attend, (row_queries, routes))
    attended = from_regions(blended.reshape(NRR * NRC, RS * RS, channels), RS, height, grid_width)
    combined = (attended + context).astype(jnp.bfloat16)
    projected_out = jnp.dot(combined.reshape(-1, channels), out_weight, preferred_element_type=jnp.float32)
    residual = image.astype(jnp.float32) + projected_out.reshape(height, grid_width, channels)
    stored = lax.optimization_barrier(residual.astype(jnp.bfloat16))
    second = layer_norm(stored, mlp_gain).astype(jnp.bfloat16)
    hidden = jax.nn.gelu(jnp.dot(second.reshape(-1, channels), up_weight, preferred_element_type=jnp.float32), approximate=True).astype(jnp.bfloat16)
    lowered = jnp.dot(hidden, down_weight, preferred_element_type=jnp.float32).reshape(height, grid_width, channels)
    return (stored.astype(jnp.float32) + lowered).astype(jnp.bfloat16)
```

```python
import functools
import itertools
import math

import jax
import jax.numpy as jnp
from jax import lax
from jax.experimental import pallas as pl
from jax.experimental.pallas import tpu as pltpu
from jax.sharding import PartitionSpec as P

MESH = pl.DeviceIdType.MESH
HEADS = 4
EPSILON = 1e-06
BIG = 1 << 20


def hops(offset):
    return sum(min(step, 4 - step) for step in offset[1:])


OFFSETS = sorted(
    (o for o in itertools.product(range(2), range(4), range(4), range(4)) if any(o)), key=hops
)


def layer_norm(floats, gain):
    centered = floats - jnp.mean(floats, axis=-1, keepdims=True)
    spread = jnp.mean(centered * centered, axis=-1, keepdims=True)
    return centered * lax.rsqrt(spread + EPSILON) * gain


def owner_of(route):
    return ((route >> 9) << 4) | ((route >> 3) & 15)


def local_of(route):
    return (((route >> 7) & 3) << 3) | (route & 7)


def to_strip(blocks):
    return blocks.reshape(8, 8, 8, 128).transpose(1, 0, 2, 3).reshape(8, 64, 128)


def exchange_kernel(
    routes_ref, image_ref, gain_ref, qkv_ref, lce_ref,
    recv_ref, q_ref, ctx_ref, pos_ref,
    normed, send, my_routes, all_routes, slots, slots_smem, grid_v, padded,
    route_send, route_recv, halo_send, halo_recv, data_send, data_recv, local_sem,
):
    row, col = lax.axis_index("rows"), lax.axis_index("cols")
    chip_y, core = row // 2, row % 2
    chip_z, chip_x = col // 4, col % 4
    me = row * 16 + col

    def peer(offset):
        dc, dy, dz, dx = offset
        return (
            (chip_y + dy) % 4 * 2 + (core + dc) % 2,
            (chip_z + dz) % 4 * 4 + (chip_x + dx) % 4,
        )

    barrier = pltpu.get_barrier_semaphore()
    for offset in reversed(OFFSETS):
        pl.semaphore_signal(barrier, inc=1, device_id=peer(offset), device_id_type=MESH)

    mine = jnp.concatenate(
        [routes_ref[i, t : t + 1, :] for i in range(4) for t in range(4)], axis=1
    )
    my_routes[...] = mine
    all_routes[pl.ds(me, 1), :] = mine

    lanes = lax.broadcasted_iota(jnp.int32, (128, 128), 1)
    subs = lax.broadcasted_iota(jnp.int32, (128, 128), 0)
    owners = jnp.broadcast_to(owner_of(mine), (128, 128))
    same = jnp.logical_and(owners == owners.T, subs < lanes)
    second = jnp.max(jnp.where(same, 1, 0), axis=0, keepdims=True)
    pos_ref[...] = owner_of(mine) * 2 + second

    gain = gain_ref[...]
    for i in range(4):
        strip = image_ref[pl.ds(8 * i, 8)].astype(jnp.float32)
        strip = to_strip(layer_norm(strip, gain)).astype(jnp.bfloat16)
        normed[pl.ds(8 * i, 8)] = strip
        projected = jnp.dot(
            strip.reshape(512, 128), qkv_ref[...], preferred_element_type=jnp.float32
        )
        q_ref[pl.ds(8 * i, 8)] = projected[:, :128].astype(jnp.bfloat16).reshape(8, 64, 128)
        values = projected[:, 256:].reshape(8, 8, 8, 128).transpose(1, 0, 2, 3)
        grid_v[pl.ds(2 + 8 * i, 8), pl.ds(1, 8)] = values.astype(jnp.bfloat16)

    pl.semaphore_wait(barrier, len(OFFSETS))

    route_copies = []
    for n, offset in enumerate(OFFSETS[::-1]):
        route_copies.append(
            pltpu.make_async_remote_copy(
                src_ref=my_routes,
                dst_ref=all_routes.at[pl.ds(me, 1)],
                send_sem=route_send.at[n],
                recv_sem=route_recv.at[n],
                device_id=peer(offset),
                device_id_type=MESH,
            )
        )
        route_copies[-1].start()

    halo_copies = []
    for n, (dr, dc) in enumerate(
        (dr, dc) for dr in (-1, 0, 1) for dc in (-1, 0, 1) if (dr, dc) != (0, 0)
    ):
        rows = {-1: (2, 34, 2), 0: (2, 2, 32), 1: (32, 0, 2)}[dr]
        cols = {-1: (1, 9, 1), 0: (1, 1, 8), 1: (8, 0, 1)}[dc]
        halo_copies.append(
            pltpu.make_async_remote_copy(
                src_ref=grid_v.at[pl.ds(rows[0], rows[2]), pl.ds(cols[0], cols[2])],
                dst_ref=grid_v.at[pl.ds(rows[1], rows[2]), pl.ds(cols[1], cols[2])],
                send_sem=halo_send.at[n],
                recv_sem=halo_recv.at[n],
                device_id=((row + dr + 8) % 8, (col + dc + 16) % 16),
                device_id_type=MESH,
            )
        )
        halo_copies[-1].start()

    for copy in route_copies:
        copy.wait()

    table = all_routes[...].T
    keys = subs * 32 + local_of(table)
    hits = owner_of(table) == me
    first = jnp.min(jnp.where(hits, keys, BIG), axis=0, keepdims=True) & 31
    last = jnp.max(jnp.where(hits, keys, 0), axis=0, keepdims=True) & 31
    slots[pl.ds(0, 1), :] = first
    slots[pl.ds(1, 1), :] = last
    to_scalars = pltpu.make_async_copy(slots, slots_smem, local_sem.at[0])
    to_scalars.start()
    to_scalars.wait()

    def fill(target):
        for s in range(2):
            send[2 * target + s] = normed[slots_smem[s, target]]

    data_copies = []

    def launch(n):
        target = peer(OFFSETS[n])
        number = target[0] * 16 + target[1]
        data_copies.append(
            pltpu.make_async_remote_copy(
                src_ref=send.at[pl.ds(2 * number, 2)],
                dst_ref=recv_ref.at[pl.ds(2 * me, 2)],
                send_sem=data_send.at[n],
                recv_sem=data_recv.at[n],
                device_id=target,
                device_id_type=MESH,
            )
        )
        data_copies[-1].start()

    lag = 2
    for n, offset in enumerate(OFFSETS):
        target = peer(offset)
        fill(target[0] * 16 + target[1])
        if n >= lag:
            launch(n - lag)
    for s in range(2):
        recv_ref[2 * me + s] = normed[slots_smem[s, me]]
    for n in range(len(OFFSETS) - lag, len(OFFSETS)):
        launch(n)

    for copy in halo_copies:
        copy.wait()
    keep_top, keep_bottom = row > 0, row < 7
    keep_left, keep_right = col > 0, col < 15

    def widen(block, keep):
        return jnp.where(keep, block.astype(jnp.float32), 0.0)

    @pl.loop(0, 36)
    def _(i):
        inside = jnp.logical_and(
            jnp.logical_or(i >= 2, keep_top), jnp.logical_or(i < 34, keep_bottom)
        )
        for j in range(10):
            keep = inside
            if j == 0:
                keep = jnp.logical_and(inside, keep_left)
            if j == 9:
                keep = jnp.logical_and(inside, keep_right)
            padded[i, pl.ds(8 * j, 8), :] = widen(grid_v[i, j], keep)

    @pl.loop(0, 8)
    def _(j):
        weights = [[lce_ref[a, pl.ds(b, 1), :] for b in range(5)] for a in range(5)]
        for i in range(4):
            totals = [None] * 8
            for line in range(12):
                for b in range(5):
                    window = padded[8 * i + line, pl.ds(8 * j + 6 + b, 8), :]
                    for a in range(5):
                        t = line - a
                        if 0 <= t < 8:
                            term = window * weights[a][b]
                            totals[t] = term if totals[t] is None else totals[t] + term
            for t in range(8):
                ctx_ref[8 * i + j, pl.ds(8 * t, 8), :] = totals[t]

    for copy in data_copies:
        copy.wait()


def exchange(routes, image, gain, qkv, lce):
    vmem = pl.BlockSpec(memory_space=pltpu.VMEM)
    dma = pltpu.SemaphoreType.DMA
    return pl.pallas_call(
        exchange_kernel,
        out_shape=(
            jax.ShapeDtypeStruct((256, 64, 128), jnp.bfloat16),
            jax.ShapeDtypeStruct((32, 64, 128), jnp.bfloat16),
            jax.ShapeDtypeStruct((32, 64, 128), jnp.float32),
            jax.ShapeDtypeStruct((1, 128), jnp.int32),
        ),
        in_specs=[vmem] * 5,
        out_specs=(vmem,) * 4,
        scratch_shapes=[
            pltpu.VMEM((32, 64, 128), jnp.bfloat16),
            pltpu.VMEM((256, 64, 128), jnp.bfloat16),
            pltpu.VMEM((1, 128), jnp.int32),
            pltpu.VMEM((128, 128), jnp.int32),
            pltpu.VMEM((2, 128), jnp.int32),
            pltpu.SMEM((2, 128), jnp.int32),
            pltpu.VMEM((36, 10, 8, 128), jnp.bfloat16),
            pltpu.VMEM((36, 80, 128), jnp.float32),
            dma((127,)), dma((127,)), dma((8,)), dma((8,)), dma((127,)), dma((127,)), dma((1,)),
        ],
        compiler_params=pltpu.CompilerParams(
            collective_id=0, has_side_effects=True, vmem_limit_bytes=40 << 20
        ),
        name="exchange",
    )(routes, image, gain, qkv, lce)


def attend_kernel(
    pos_ref, recv_ref, q_ref, ctx_ref, image_ref, key_ref, value_ref, out_w_ref, gain_ref,
    up_ref, down_ref, out_ref, combined,
):
    factor = 32 ** (-0.5) / math.log(2)
    lane_head = lax.broadcasted_iota(jnp.int32, (64, 128), 1) // 32
    low_lanes = lax.broadcasted_iota(jnp.int32, (32, 128), 1) < 64
    over_last = (((1,), (1,)), ((), ()))

    def attend(r, parity):
        base = (r // 8) * 32 + r % 8
        tokens = jnp.concatenate([recv_ref[pos_ref[0, base + 8 * t]] for t in range(4)], axis=0)
        keys = jnp.dot(tokens, key_ref[...], preferred_element_type=jnp.float32)
        values = lax.dot_general(
            value_ref[...], tokens, over_last, preferred_element_type=jnp.float32
        )
        queries = q_ref[r]
        zero = jnp.zeros_like(queries)
        stacked = jnp.concatenate(
            [jnp.where(lane_head == h, queries, zero) for h in range(HEADS)], axis=0
        )
        scores = lax.dot_general(
            keys.astype(jnp.bfloat16), stacked, over_last, preferred_element_type=jnp.float32
        )
        expons = jnp.exp2((scores - jnp.max(scores, axis=0, keepdims=True)) * factor)
        weights = expons * (1.0 / jnp.sum(expons, axis=0, keepdims=True))
        blended = jnp.dot(
            values.astype(jnp.bfloat16), weights.astype(jnp.bfloat16),
            preferred_element_type=jnp.float32,
        )
        parts = []
        for h in range(HEADS):
            part = blended[32 * h : 32 * h + 32, 128 * (h // 2) : 128 * (h // 2) + 128]
            if h % 2 != parity:
                part = pltpu.roll(part, 64, 1)
            parts.append(part)
        return parts

    @pl.loop(0, 16)
    def _(p):
        even, odd = attend(2 * p, 0), attend(2 * p + 1, 1)
        both = jnp.concatenate([jnp.where(low_lanes, a, b) for a, b in zip(even, odd)], axis=0)
        attended = both.T.reshape(2, 64, 128)
        combined[pl.ds(2 * p, 2)] = (attended + ctx_ref[pl.ds(2 * p, 2)]).astype(jnp.bfloat16)

    @pl.loop(0, 4)
    def _(i):
        strip = to_strip(image_ref[pl.ds(8 * i, 8)].astype(jnp.float32)).reshape(512, 128)
        mixed = jnp.dot(
            combined[pl.ds(8 * i, 8)].reshape(512, 128), out_w_ref[...],
            preferred_element_type=jnp.float32,
        )
        stored = (strip + mixed).astype(jnp.bfloat16).astype(jnp.float32)
        second = layer_norm(stored, gain_ref[...]).astype(jnp.bfloat16)
        lifted = jnp.dot(second, up_ref[...], preferred_element_type=jnp.float32)
        hidden = jax.nn.gelu(lifted, approximate=True).astype(jnp.bfloat16)
        lowered = jnp.dot(hidden, down_ref[...], preferred_element_type=jnp.float32)
        refined = (stored + lowered).reshape(8, 64, 128)
        out_ref[pl.ds(8 * i, 8)] = to_strip(refined).astype(jnp.bfloat16)


def attend(pos, recv, q, ctx, image, key_w, value_w, out_w, gain, up, down):
    vmem = pl.BlockSpec(memory_space=pltpu.VMEM)
    return pl.pallas_call(
        attend_kernel,
        out_shape=jax.ShapeDtypeStruct((32, 64, 128), jnp.bfloat16),
        in_specs=[pl.BlockSpec(memory_space=pltpu.SMEM)] + [vmem] * 10,
        out_specs=vmem,
        scratch_shapes=[pltpu.VMEM((32, 64, 128), jnp.bfloat16)],
        compiler_params=pltpu.CompilerParams(vmem_limit_bytes=40 << 20),
        name="attend",
    )(pos, recv, q, ctx, image, key_w, value_w, out_w, gain, up, down)


def body(
    image, routes, norm_gain, qkv_weight, lce_weight, out_weight, mlp_gain, up_weight, down_weight
):
    recv, q, ctx, pos = exchange(
        routes.transpose(0, 2, 1), image, norm_gain[None], qkv_weight, lce_weight
    )
    return attend(
        pos, recv, q, ctx, image, qkv_weight[:, 128:256], qkv_weight[:, 256:].T, out_weight,
        mlp_gain[None], up_weight, down_weight,
    )


def solution(mesh):
    in_specs = (P("rows", "cols", None), P("rows", "cols", None), P(), P(), P(), P(), P(), P(), P())
    out_specs = P("rows", "cols", None)
    return jax.shard_map(body, mesh=mesh, in_specs=in_specs, out_specs=out_specs, check_vma=False)
```

```python
import functools
import itertools
import math

import jax
import jax.numpy as jnp
from jax import lax
from jax.experimental import pallas as pl
from jax.experimental.pallas import tpu as pltpu
from jax.sharding import PartitionSpec as P

MESH = pl.DeviceIdType.MESH
HEADS = 4
EPSILON = 1e-06
BIG = 1 << 20


def hops(offset):
    return sum(min(step, 4 - step) for step in offset[1:])


OFFSETS = sorted(
    (o for o in itertools.product(range(2), range(4), range(4), range(4)) if any(o)), key=hops
)


def layer_norm(floats, gain):
    centered = floats - jnp.mean(floats, axis=-1, keepdims=True)
    spread = jnp.mean(centered * centered, axis=-1, keepdims=True)
    return centered * lax.rsqrt(spread + EPSILON) * gain


def owner_of(route):
    return ((route >> 9) << 4) | ((route >> 3) & 15)


def local_of(route):
    return (((route >> 7) & 3) << 3) | (route & 7)


def to_strip(blocks):
    return blocks.reshape(8, 8, 8, 128).transpose(1, 0, 2, 3).reshape(8, 64, 128)


def block_kernel(
    image_hbm, routes_hbm, norm_gain_hbm, qkv_hbm, lce_hbm, out_w_hbm, mlp_gain_hbm, up_hbm, down_hbm,
    out_hbm,
    image_ref, routes_ref, norm_gain_ref, qkv_ref, lce_ref, out_w_ref, mlp_gain_ref, up_ref, down_ref,
    normed, send, recv, keys_ref, values_ref, queries_ref, ctx_ref, combined, refined_ref,
    my_routes, all_routes, slots, slots_smem, place, place_smem, grid_v, padded,
    load_sem, route_send, route_recv, halo_send, halo_recv, data_send, data_recv, local_sem, out_sem,
):
    row, col = lax.axis_index("rows"), lax.axis_index("cols")
    chip_y, core = row // 2, row % 2
    chip_z, chip_x = col // 4, col % 4
    me = row * 16 + col
    over_last = (((1,), (1,)), ((), ()))
    over_first = (((0,), (0,)), ((), ()))

    def peer(offset):
        dc, dy, dz, dx = offset
        return (
            (chip_y + dy) % 4 * 2 + (core + dc) % 2,
            (chip_z + dz) % 4 * 4 + (chip_x + dx) % 4,
        )

    pairs = [
        (image_hbm, image_ref), (routes_hbm, routes_ref), (qkv_hbm, qkv_ref),
        (norm_gain_hbm, norm_gain_ref), (lce_hbm, lce_ref), (out_w_hbm, out_w_ref),
        (mlp_gain_hbm, mlp_gain_ref), (up_hbm, up_ref), (down_hbm, down_ref),
    ]
    loads = [pltpu.make_async_copy(a, b, load_sem.at[n]) for n, (a, b) in enumerate(pairs)]
    for load in loads:
        load.start()
    barrier = pltpu.get_barrier_semaphore()
    for offset in reversed(OFFSETS):
        pl.semaphore_signal(barrier, inc=1, device_id=peer(offset), device_id_type=MESH)
    for load in loads:
        load.wait()

    mine = jnp.concatenate(
        [routes_ref[i, t : t + 1, :] for i in range(4) for t in range(4)], axis=1
    )
    my_routes[...] = mine
    all_routes[pl.ds(me, 1), :] = mine

    gain = norm_gain_ref[...]
    for i in range(4):
        strip = image_ref[pl.ds(8 * i, 8)].astype(jnp.float32)
        strip = to_strip(layer_norm(strip, gain)).astype(jnp.bfloat16)
        normed[pl.ds(8 * i, 8)] = strip
        values = jnp.dot(
            strip.reshape(512, 128), qkv_ref[:, 256:384], preferred_element_type=jnp.float32
        )
        values = values.reshape(8, 8, 8, 128).transpose(1, 0, 2, 3)
        grid_v[pl.ds(2 + 8 * i, 8), pl.ds(1, 8)] = values.astype(jnp.bfloat16)

    lanes = lax.broadcasted_iota(jnp.int32, (128, 128), 1)
    subs = lax.broadcasted_iota(jnp.int32, (128, 128), 0)
    owners = jnp.broadcast_to(owner_of(mine), (128, 128))
    same = jnp.logical_and(owners == owners.T, subs < lanes)
    second = jnp.max(jnp.where(same, 1, 0), axis=0, keepdims=True)
    place[...] = owner_of(mine) * 2 + second
    to_places = pltpu.make_async_copy(place, place_smem, local_sem.at[1])
    to_places.start()

    pl.semaphore_wait(barrier, len(OFFSETS))

    route_copies = []
    for n, offset in enumerate(OFFSETS[::-1]):
        route_copies.append(
            pltpu.make_async_remote_copy(
                src_ref=my_routes,
                dst_ref=all_routes.at[pl.ds(me, 1)],
                send_sem=route_send.at[n],
                recv_sem=route_recv.at[n],
                device_id=peer(offset),
                device_id_type=MESH,
            )
        )
        route_copies[-1].start()

    halo_copies = []
    for n, (dr, dc) in enumerate(
        (dr, dc) for dr in (-1, 0, 1) for dc in (-1, 0, 1) if (dr, dc) != (0, 0)
    ):
        rows = {-1: (2, 34, 2), 0: (2, 2, 32), 1: (32, 0, 2)}[dr]
        cols = {-1: (1, 9, 1), 0: (1, 1, 8), 1: (8, 0, 1)}[dc]
        halo_copies.append(
            pltpu.make_async_remote_copy(
                src_ref=grid_v.at[pl.ds(rows[0], rows[2]), pl.ds(cols[0], cols[2])],
                dst_ref=grid_v.at[pl.ds(rows[1], rows[2]), pl.ds(cols[1], cols[2])],
                send_sem=halo_send.at[n],
                recv_sem=halo_recv.at[n],
                device_id=((row + dr + 8) % 8, (col + dc + 16) % 16),
                device_id_type=MESH,
            )
        )
        halo_copies[-1].start()

    for copy in route_copies:
        copy.wait()

    table = all_routes[...].T
    order = subs * 32 + local_of(table)
    hits = owner_of(table) == me
    first = jnp.min(jnp.where(hits, order, BIG), axis=0, keepdims=True) & 31
    last = jnp.max(jnp.where(hits, order, 0), axis=0, keepdims=True) & 31
    slots[pl.ds(0, 1), :] = first
    slots[pl.ds(1, 1), :] = last
    to_scalars = pltpu.make_async_copy(slots, slots_smem, local_sem.at[0])
    to_scalars.start()
    to_scalars.wait()

    def fill(target):
        for s in range(2):
            send[2 * target + s] = normed[slots_smem[s, target]]

    data_copies = []

    def launch(n):
        target = peer(OFFSETS[n])
        number = target[0] * 16 + target[1]
        data_copies.append(
            pltpu.make_async_remote_copy(
                src_ref=send.at[pl.ds(2 * number, 2)],
                dst_ref=recv.at[pl.ds(2 * me, 2)],
                send_sem=data_send.at[n],
                recv_sem=data_recv.at[n],
                device_id=target,
                device_id_type=MESH,
            )
        )
        data_copies[-1].start()

    lag = 2
    for n, offset in enumerate(OFFSETS):
        target = peer(offset)
        fill(target[0] * 16 + target[1])
        if n >= lag:
            launch(n - lag)
    for s in range(2):
        recv[2 * me + s] = normed[slots_smem[s, me]]
    for n in range(len(OFFSETS) - lag, len(OFFSETS)):
        launch(n)

    query_w = qkv_ref[:, 0:128].T
    feature_head = lax.broadcasted_iota(jnp.int32, (128, 256), 0) // 32
    across_head = lax.broadcasted_iota(jnp.int32, (128, 256), 1) // 64
    own_head = feature_head == across_head

    @pl.loop(0, 32)
    def _(r):
        tokens = normed[r]
        wide = lax.dot_general(
            query_w, jnp.concatenate([tokens] * 4, axis=0), over_last,
            preferred_element_type=jnp.float32,
        )
        queries_ref[r] = jnp.where(own_head, wide, 0.0).astype(jnp.bfloat16)

    for copy in halo_copies:
        copy.wait()
    keep_top, keep_bottom = row > 0, row < 7
    keep_left, keep_right = col > 0, col < 15

    @pl.loop(0, 36)
    def _(i):
        inside = jnp.logical_and(
            jnp.logical_or(i >= 2, keep_top), jnp.logical_or(i < 34, keep_bottom)
        )
        for j in range(10):
            keep = inside
            if j == 0:
                keep = jnp.logical_and(inside, keep_left)
            if j == 9:
                keep = jnp.logical_and(inside, keep_right)
            padded[i, pl.ds(8 * j, 8), :] = jnp.where(keep, grid_v[i, j].astype(jnp.float32), 0.0)

    @pl.loop(0, 8)
    def _(j):
        weights = [[lce_ref[a, pl.ds(b, 1), :] for b in range(5)] for a in range(5)]
        for i in range(4):
            totals = [None] * 8
            for line in range(12):
                for b in range(5):
                    window = padded[8 * i + line, pl.ds(8 * j + 6 + b, 8), :]
                    for a in range(5):
                        t = line - a
                        if 0 <= t < 8:
                            term = window * weights[a][b]
                            totals[t] = term if totals[t] is None else totals[t] + term
            for t in range(8):
                ctx_ref[8 * i + j, pl.ds(8 * t, 8), :] = totals[t]

    def project(source):
        tokens = recv[pl.ds(2 * source, 2)].reshape(128, 128)
        both = jnp.dot(tokens, qkv_ref[:, 128:384], preferred_element_type=jnp.float32)
        both = both.astype(jnp.bfloat16)
        keys_ref[pl.ds(2 * source, 2)] = both[:, :128].reshape(2, 64, 128)
        values_ref[pl.ds(2 * source, 2)] = both[:, 128:].reshape(2, 64, 128)

    project(me)
    for n, offset in enumerate(OFFSETS):
        dc, dy, dz, dx = offset
        source = peer((dc, 4 - dy, 4 - dz, 4 - dx))
        data_copies[n].wait_recv()
        project(source[0] * 16 + source[1])
    to_places.wait()

    factor = 32 ** (-0.5) / math.log(2)
    low_lanes = lax.broadcasted_iota(jnp.int32, (32, 128), 1) < 64

    def attend(r, parity):
        base = (r // 8) * 32 + r % 8
        spots = [place_smem[0, base + 8 * t] for t in range(4)]
        keys = jnp.concatenate([keys_ref[s] for s in spots], axis=0)
        values = jnp.concatenate([values_ref[s] for s in spots], axis=0)
        scores = jnp.dot(keys, queries_ref[r], preferred_element_type=jnp.float32)
        expons = jnp.exp2((scores - jnp.max(scores, axis=0, keepdims=True)) * factor)
        weights = expons * (1.0 / jnp.sum(expons, axis=0, keepdims=True))
        blended = lax.dot_general(
            values, weights.astype(jnp.bfloat16), over_first, preferred_element_type=jnp.float32
        )
        parts = []
        for h in range(HEADS):
            part = blended[32 * h : 32 * h + 32, 128 * (h // 2) : 128 * (h // 2) + 128]
            if h % 2 != parity:
                part = pltpu.roll(part, 64, 1)
            parts.append(part)
        return parts

    @pl.loop(0, 32 // GROUP)
    def _(g):
        for p in range(GROUP // 2):
            r = g * GROUP + 2 * p
            even, odd = attend(r, 0), attend(r + 1, 1)
            both = jnp.concatenate([jnp.where(low_lanes, a, b) for a, b in zip(even, odd)], axis=0)
            attended = both.T.reshape(2, 64, 128)
            combined[pl.ds(r, 2)] = (attended + ctx_ref[pl.ds(r, 2)]).astype(jnp.bfloat16)

    @pl.loop(0, 4)
    def _(i):
        strip = to_strip(image_ref[pl.ds(8 * i, 8)].astype(jnp.float32)).reshape(512, 128)
        mixed = jnp.dot(
            combined[pl.ds(8 * i, 8)].reshape(512, 128), out_w_ref[...],
            preferred_element_type=jnp.float32,
        )
        stored = (strip + mixed).astype(jnp.bfloat16).astype(jnp.float32)
        second = layer_norm(stored, mlp_gain_ref[...]).astype(jnp.bfloat16)
        lifted = jnp.dot(second, up_ref[...], preferred_element_type=jnp.float32)
        hidden = jax.nn.gelu(lifted, approximate=True).astype(jnp.bfloat16)
        lowered = jnp.dot(hidden, down_ref[...], preferred_element_type=jnp.float32)
        refined = (stored + lowered).reshape(8, 64, 128)
        refined_ref[pl.ds(8 * i, 8)] = to_strip(refined).astype(jnp.bfloat16)

    store = pltpu.make_async_copy(refined_ref, out_hbm, out_sem)
    store.start()
    for copy in data_copies:
        copy.wait_send()
    store.wait()


GROUP = 4


def body(
    image, routes, norm_gain, qkv_weight, lce_weight, out_weight, mlp_gain, up_weight, down_weight
):
    operands = (
        image, routes.transpose(0, 2, 1), norm_gain[None], qkv_weight, lce_weight, out_weight,
        mlp_gain[None], up_weight, down_weight,
    )
    hbm = pl.BlockSpec(memory_space=pl.ANY)
    dma = pltpu.SemaphoreType.DMA
    bf16, f32, i32 = jnp.bfloat16, jnp.float32, jnp.int32
    return pl.pallas_call(
        block_kernel,
        out_shape=jax.ShapeDtypeStruct((32, 64, 128), bf16),
        in_specs=[hbm] * 9,
        out_specs=hbm,
        scratch_shapes=[pltpu.VMEM(x.shape, x.dtype) for x in operands] + [
            pltpu.VMEM((32, 64, 128), bf16),
            pltpu.VMEM((256, 64, 128), bf16),
            pltpu.VMEM((256, 64, 128), bf16),
            pltpu.VMEM((256, 64, 128), bf16),
            pltpu.VMEM((256, 64, 128), bf16),
            pltpu.VMEM((32, 128, 256), bf16),
            pltpu.VMEM((32, 64, 128), f32),
            pltpu.VMEM((32, 64, 128), bf16),
            pltpu.VMEM((32, 64, 128), bf16),
            pltpu.VMEM((1, 128), i32),
            pltpu.VMEM((128, 128), i32),
            pltpu.VMEM((2, 128), i32),
            pltpu.SMEM((2, 128), i32),
            pltpu.VMEM((1, 128), i32),
            pltpu.SMEM((1, 128), i32),
            pltpu.VMEM((36, 10, 8, 128), bf16),
            pltpu.VMEM((36, 80, 128), f32),
            dma((9,)), dma((127,)), dma((127,)), dma((8,)), dma((8,)), dma((127,)), dma((127,)),
            dma((2,)), dma(()),
        ],
        compiler_params=pltpu.CompilerParams(
            collective_id=0, has_side_effects=True, vmem_limit_bytes=60 << 20
        ),
        name="block",
    )(*operands)


def solution(mesh):
    in_specs = (P("rows", "cols", None), P("rows", "cols", None), P(), P(), P(), P(), P(), P(), P())
    out_specs = P("rows", "cols", None)
    return jax.shard_map(body, mesh=mesh, in_specs=in_specs, out_specs=out_specs, check_vma=False)
```

```python
import functools
import itertools
import math

import jax
import jax.numpy as jnp
from jax import lax
from jax.experimental import pallas as pl
from jax.experimental.pallas import tpu as pltpu
from jax.sharding import PartitionSpec as P

MESH = pl.DeviceIdType.MESH
HEADS = 4
EPSILON = 1e-06
BIG = 1 << 20


def hops(offset):
    return sum(min(step, 4 - step) for step in offset[1:])


OFFSETS = sorted(
    (o for o in itertools.product(range(2), range(4), range(4), range(4)) if any(o)), key=hops
)


PART = 16
PLANE = sorted(
    (o for o in itertools.product(range(2), range(4), range(4)) if any(o)), key=hops
)
BATCHES = (range(0, 8), range(8, 16), range(16, 22), range(22, 27), range(27, 31))
BATCH_OF = [b for b, members in enumerate(BATCHES) for _ in members]


def widened(part, offset):
    dc, first, second = offset
    return ((dc, first, second, 0), (dc, 0, second, first), (dc, first, 0, second))[part]


def layer_norm(floats, gain):
    centered = floats - jnp.mean(floats, axis=-1, keepdims=True)
    spread = jnp.mean(centered * centered, axis=-1, keepdims=True)
    return centered * lax.rsqrt(spread + EPSILON) * gain


def owner_of(route):
    return ((route >> 9) << 4) | ((route >> 3) & 15)


def local_of(route):
    return (((route >> 7) & 3) << 3) | (route & 7)


def to_strip(blocks):
    return blocks.reshape(8, 8, 8, 128).transpose(1, 0, 2, 3).reshape(8, 64, 128)


def block_kernel(
    image_hbm, routes_hbm, norm_gain_hbm, qkv_hbm, lce_hbm, out_w_hbm, mlp_gain_hbm, up_hbm, down_hbm,
    refined_ref,
    image_ref, routes_ref, norm_gain_ref, qkv_ref, lce_ref, out_w_ref, mlp_gain_ref, up_ref, down_ref,
    lines, straight, send, recv, keys_ref, values_ref, queries_ref, ctx_ref, combined,
    my_routes, all_routes, slots, slots_smem, place, place_smem, grid_v, padded,
    load_sem, send_sem, recv_sem, local_sem,
):
    row, col = lax.axis_index("rows"), lax.axis_index("cols")
    chip_y, core = row // 2, row % 2
    chip_z, chip_x = col // 4, col % 4
    me = row * 16 + col
    spots = (chip_x, chip_y, chip_z)
    relays = (
        (core * 4 + chip_z) * 4 + chip_y,
        (core * 4 + chip_z) * 4 + chip_x,
        (core * 4 + chip_y) * 4 + chip_x,
    )
    over_last = (((1,), (1,)), ((), ()))
    over_first = (((0,), (0,)), ((), ()))

    def peer(offset):
        dc, dy, dz, dx = offset
        return (
            (chip_y + dy) % 4 * 2 + (core + dc) % 2,
            (chip_z + dz) % 4 * 4 + (chip_x + dx) % 4,
        )

    pairs = [
        (image_hbm, image_ref), (routes_hbm, routes_ref), (qkv_hbm, qkv_ref),
        (norm_gain_hbm, norm_gain_ref), (lce_hbm, lce_ref), (out_w_hbm, out_w_ref),
        (mlp_gain_hbm, mlp_gain_ref), (up_hbm, up_ref), (down_hbm, down_ref),
    ]
    loads = [pltpu.make_async_copy(a, b, load_sem.at[n]) for n, (a, b) in enumerate(pairs)]
    for load in loads:
        load.start()
    barrier = pltpu.get_barrier_semaphore()
    for offset in reversed(OFFSETS):
        pl.semaphore_signal(barrier, inc=1, device_id=peer(offset), device_id_type=MESH)
    for load in loads:
        load.wait()

    mine = jnp.concatenate(
        [routes_ref[i, t : t + 1, :] for i in range(4) for t in range(4)], axis=1
    )
    my_routes[...] = mine
    all_routes[pl.ds(me, 1), :] = mine

    gain = norm_gain_ref[...]
    for i in range(4):
        strip = image_ref[pl.ds(8 * i, 8)].astype(jnp.float32)
        strip = to_strip(layer_norm(strip, gain)).astype(jnp.bfloat16)
        for p in range(3):
            lines[p][spots[p], pl.ds(8 * i, 8)] = strip[:, PART * p : PART * p + PART]
        straight[pl.ds(8 * i, 8)] = strip[:, PART * 3 :]
        values = jnp.dot(
            strip.reshape(512, 128), qkv_ref[:, 256:384], preferred_element_type=jnp.float32
        )
        values = values.reshape(8, 8, 8, 128).transpose(1, 0, 2, 3)
        grid_v[pl.ds(2 + 8 * i, 8), pl.ds(1, 8)] = values.astype(jnp.bfloat16)

    lanes = lax.broadcasted_iota(jnp.int32, (128, 128), 1)
    subs = lax.broadcasted_iota(jnp.int32, (128, 128), 0)
    owners = jnp.broadcast_to(owner_of(mine), (128, 128))
    same = jnp.logical_and(owners == owners.T, subs < lanes)
    second = jnp.max(jnp.where(same, 1, 0), axis=0, keepdims=True)
    own = owner_of(mine)
    oy, oc, oz, ox = own >> 5, (own >> 4) & 1, (own >> 2) & 3, own & 3
    place[pl.ds(0, 1), :] = ((oc * 4 + oz) * 4 + oy) * 8 + ox * 2 + second
    place[pl.ds(1, 1), :] = ((oc * 4 + oz) * 4 + ox) * 8 + oy * 2 + second
    place[pl.ds(2, 1), :] = ((oc * 4 + oy) * 4 + ox) * 8 + oz * 2 + second
    place[pl.ds(3, 1), :] = own * 2 + second
    to_places = pltpu.make_async_copy(place, place_smem, local_sem.at[1])
    to_places.start()

    pl.semaphore_wait(barrier, len(OFFSETS))

    route_copies = []
    for n, offset in enumerate(OFFSETS[::-1]):
        route_copies.append(
            pltpu.make_async_remote_copy(
                src_ref=my_routes,
                dst_ref=all_routes.at[pl.ds(me, 1)],
                send_sem=send_sem.at[0],
                recv_sem=recv_sem.at[0],
                device_id=peer(offset),
                device_id_type=MESH,
            )
        )
        route_copies[-1].start()

    halo_copies = []
    for n, (dr, dc) in enumerate(
        (dr, dc) for dr in (-1, 0, 1) for dc in (-1, 0, 1) if (dr, dc) != (0, 0)
    ):
        rows = {-1: (2, 34, 2), 0: (2, 2, 32), 1: (32, 0, 2)}[dr]
        cols = {-1: (1, 9, 1), 0: (1, 1, 8), 1: (8, 0, 1)}[dc]
        halo_copies.append(
            pltpu.make_async_remote_copy(
                src_ref=grid_v.at[pl.ds(rows[0], rows[2]), pl.ds(cols[0], cols[2])],
                dst_ref=grid_v.at[pl.ds(rows[1], rows[2]), pl.ds(cols[1], cols[2])],
                send_sem=send_sem.at[1],
                recv_sem=recv_sem.at[1 + n],
                device_id=((row + dr + 8) % 8, (col + dc + 16) % 16),
                device_id_type=MESH,
            )
        )
        halo_copies[-1].start()

    line_copies = []
    for p in range(3):
        for step in (1, 3, 2):
            offset = tuple(step if axis == 3 - (0, 2, 1)[p] else 0 for axis in range(4))
            line_copies.append(
                pltpu.make_async_remote_copy(
                    src_ref=lines[p].at[spots[p]],
                    dst_ref=lines[p].at[spots[p]],
                    send_sem=send_sem.at[2 + p],
                    recv_sem=recv_sem.at[9 + p],
                    device_id=peer(offset),
                    device_id_type=MESH,
                )
            )
            line_copies[-1].start()

    query_w = qkv_ref[:, 0:128].T
    feature_head = lax.broadcasted_iota(jnp.int32, (128, 256), 0) // 32
    across_head = lax.broadcasted_iota(jnp.int32, (128, 256), 1) // 64
    own_head = feature_head == across_head

    def lay_out(r):
        tokens = jnp.concatenate(
            [lines[p][spots[p], r] for p in range(3)] + [straight[r]], axis=0
        )
        wide = lax.dot_general(
            query_w, jnp.concatenate([tokens] * 4, axis=0), over_last,
            preferred_element_type=jnp.float32,
        )
        queries_ref[r] = jnp.where(own_head, wide, 0.0).astype(jnp.bfloat16)

    @pl.loop(0, 8)
    def _(i):
        for j in range(4):
            lay_out(4 * i + j)

    def wait_bytes(ref, sem):
        pltpu.make_async_copy(ref, ref, sem).wait()

    wait_bytes(all_routes.at[pl.ds(0, 127)], recv_sem.at[0])

    table = all_routes[...].T
    order = subs * 32 + local_of(table)
    table_owner = owner_of(table)
    for p in range(3):
        for i in range(4):
            owner = (
                row * 16 + chip_z * 4 + i,
                (i * 2 + core) * 16 + col,
                row * 16 + i * 4 + chip_x,
            )[p]
            hits = table_owner == owner
            first = jnp.min(jnp.where(hits, order, BIG), axis=0, keepdims=True) & 31
            last = jnp.max(jnp.where(hits, order, 0), axis=0, keepdims=True) & 31
            slots[pl.ds(8 * p + 2 * i, 1), :] = first
            slots[pl.ds(8 * p + 2 * i + 1, 1), :] = last
    to_scalars = pltpu.make_async_copy(slots, slots_smem, local_sem.at[0])
    to_scalars.start()
    to_scalars.wait()

    def fill(p, number, into, base):
        for i in range(4):
            for t in range(2):
                into[base + 2 * i + t] = lines[p][i, slots_smem[8 * p + 2 * i + t, number]]

    def launch(p, n):
        pltpu.make_async_remote_copy(
            src_ref=send[p].at[pl.ds(8 * n, 8)],
            dst_ref=recv[p].at[pl.ds(8 * relays[p], 8)],
            send_sem=send_sem.at[5 + p],
            recv_sem=recv_sem.at[12 + len(BATCHES) * p + BATCH_OF[n]],
            device_id=peer(widened(p, PLANE[n])),
            device_id_type=MESH,
        ).start()

    def fill_straight(number, into, base):
        for t in range(2):
            into[base + t] = straight[slots_smem[2 * chip_x + t, number]]

    def launch_straight(n):
        pltpu.make_async_remote_copy(
            src_ref=send[3].at[pl.ds(2 * n, 2)],
            dst_ref=recv[3].at[pl.ds(2 * me, 2)],
            send_sem=send_sem.at[8],
            recv_sem=recv_sem.at[12 + 3 * len(BATCHES)],
            device_id=peer(OFFSETS[n]),
            device_id_type=MESH,
        ).start()

    pending = []

    def queue(start, *which):
        pending.append((start, which))
        if len(pending) > 2:
            begin, what = pending.pop(0)
            begin(*what)

    for n, offset in enumerate(OFFSETS):
        target = peer(offset)
        fill_straight(target[0] * 16 + target[1], send[3], 2 * n)
        queue(launch_straight, n)
    for p in range(3):
        wait_bytes(lines[p].at[pl.ds(0, 3)], recv_sem.at[9 + p])
    for n in range(31):
        for p in range(3):
            target = peer(widened(p, PLANE[n]))
            fill(p, target[0] * 16 + target[1], send[p], 8 * n)
            queue(launch, p, n)
    for p in range(3):
        fill(p, me, recv[p], 8 * relays[p])
    fill_straight(me, recv[3], 2 * me)
    for begin, what in pending:
        begin(*what)

    for copy in halo_copies:
        copy.wait_recv()
    keep_top, keep_bottom = row > 0, row < 7
    keep_left, keep_right = col > 0, col < 15

    @pl.loop(0, 36)
    def _(i):
        inside = jnp.logical_and(
            jnp.logical_or(i >= 2, keep_top), jnp.logical_or(i < 34, keep_bottom)
        )
        for j in range(10):
            keep = inside
            if j == 0:
                keep = jnp.logical_and(inside, keep_left)
            if j == 9:
                keep = jnp.logical_and(inside, keep_right)
            padded[i, pl.ds(8 * j, 8), :] = jnp.where(keep, grid_v[i, j].astype(jnp.float32), 0.0)

    @pl.loop(0, 8)
    def _(j):
        weights = [[lce_ref[a, pl.ds(b, 1), :] for b in range(5)] for a in range(5)]
        for i in range(4):
            totals = [None] * 8
            for line in range(12):
                for b in range(5):
                    window = padded[8 * i + line, pl.ds(8 * j + 6 + b, 8), :]
                    for a in range(5):
                        t = line - a
                        if 0 <= t < 8:
                            term = window * weights[a][b]
                            totals[t] = term if totals[t] is None else totals[t] + term
            for t in range(8):
                ctx_ref[8 * i + j, pl.ds(8 * t, 8), :] = totals[t]

    def project(p, first, count):
        tokens = recv[p][pl.ds(first, count)].reshape(count * PART, 128)
        both = jnp.dot(tokens, qkv_ref[:, 128:384], preferred_element_type=jnp.float32)
        both = both.astype(jnp.bfloat16)
        keys_ref[p][pl.ds(first, count)] = both[:, :128].reshape(count, PART, 128)
        values_ref[p][pl.ds(first, count)] = both[:, 128:].reshape(count, PART, 128)

    for p in range(3):
        project(p, 8 * relays[p], 8)
    wait_bytes(recv[3].at[pl.ds(0, 254)], recv_sem.at[12 + 3 * len(BATCHES)])

    @pl.loop(0, 16)
    def _(i):
        project(3, 16 * i, 16)

    for batch, p in itertools.product(range(len(BATCHES)), range(3)):
        members = BATCHES[batch]
        wait_bytes(
            recv[p].at[pl.ds(0, 8 * len(members))], recv_sem.at[12 + len(BATCHES) * p + batch]
        )
        for n in members:
            dc, first, second = PLANE[n]
            y, x, z = chip_y + 4, chip_x + 4, chip_z + 4
            low, high = ((y, z), (x, z), (x, y))[p]
            if p == 2:
                first, second = second, first
            relay = ((core + dc) % 2 * 4 + (high - second) % 4) * 4 + (low - first) % 4
            project(p, 8 * relay, 8)
    to_places.wait()

    factor = 32 ** (-0.5) / math.log(2)
    low_lanes = lax.broadcasted_iota(jnp.int32, (32, 128), 1) < 64

    def attend(r, parity):
        base = (r // 8) * 32 + r % 8
        found = [(p, place_smem[p, base + 8 * t]) for t in range(4) for p in range(4)]
        keys = jnp.concatenate([keys_ref[p][s] for p, s in found], axis=0)
        values = jnp.concatenate([values_ref[p][s] for p, s in found], axis=0)
        scores = jnp.dot(keys, queries_ref[r], preferred_element_type=jnp.float32)
        expons = jnp.exp2((scores - jnp.max(scores, axis=0, keepdims=True)) * factor)
        weights = expons * (1.0 / jnp.sum(expons, axis=0, keepdims=True))
        blended = lax.dot_general(
            values, weights.astype(jnp.bfloat16), over_first, preferred_element_type=jnp.float32
        )
        parts = []
        for h in range(HEADS):
            part = blended[32 * h : 32 * h + 32, 128 * (h // 2) : 128 * (h // 2) + 128]
            if h % 2 != parity:
                part = pltpu.roll(part, 64, 1)
            parts.append(part)
        return parts

    @pl.loop(0, 32 // GROUP)
    def _(g):
        for p in range(GROUP // 2):
            r = g * GROUP + 2 * p
            even, odd = attend(r, 0), attend(r + 1, 1)
            both = jnp.concatenate([jnp.where(low_lanes, a, b) for a, b in zip(even, odd)], axis=0)
            attended = both.T.reshape(2, 64, 128)
            combined[pl.ds(r, 2)] = (attended + ctx_ref[pl.ds(r, 2)]).astype(jnp.bfloat16)

    @pl.loop(0, 4)
    def _(i):
        strip = to_strip(image_ref[pl.ds(8 * i, 8)].astype(jnp.float32)).reshape(512, 128)
        mixed = jnp.dot(
            combined[pl.ds(8 * i, 8)].reshape(512, 128), out_w_ref[...],
            preferred_element_type=jnp.float32,
        )
        stored = (strip + mixed).astype(jnp.bfloat16).astype(jnp.float32)
        second = layer_norm(stored, mlp_gain_ref[...]).astype(jnp.bfloat16)
        lifted = jnp.dot(second, up_ref[...], preferred_element_type=jnp.float32)
        hidden = jax.nn.gelu(lifted, approximate=True).astype(jnp.bfloat16)
        lowered = jnp.dot(hidden, down_ref[...], preferred_element_type=jnp.float32)
        refined = (stored + lowered).reshape(8, 64, 128)
        refined_ref[pl.ds(8 * i, 8)] = to_strip(refined).astype(jnp.bfloat16)

    wait_bytes(all_routes.at[pl.ds(0, 127)], send_sem.at[0])
    for copy in halo_copies:
        wait_bytes(copy.src_ref, send_sem.at[1])
    for p in range(3):
        wait_bytes(lines[p].at[pl.ds(0, 3)], send_sem.at[2 + p])
        wait_bytes(send[p], send_sem.at[5 + p])
    wait_bytes(send[3], send_sem.at[8])


GROUP = 8


def body(
    image, routes, norm_gain, qkv_weight, lce_weight, out_weight, mlp_gain, up_weight, down_weight
):
    operands = (
        image, routes.transpose(0, 2, 1), norm_gain[None], qkv_weight, lce_weight, out_weight,
        mlp_gain[None], up_weight, down_weight,
    )
    hbm = pl.BlockSpec(memory_space=pltpu.HBM)
    dma = pltpu.SemaphoreType.DMA
    bf16, f32, i32 = jnp.bfloat16, jnp.float32, jnp.int32
    return pl.pallas_call(
        block_kernel,
        out_shape=jax.ShapeDtypeStruct((32, 64, 128), bf16),
        in_specs=[hbm] * 9,
        out_specs=pl.BlockSpec(memory_space=pltpu.VMEM),
        scratch_shapes=[pltpu.VMEM(x.shape, x.dtype) for x in operands] + [
            [pltpu.VMEM((4, 32, PART, 128), bf16)] * 3,
            pltpu.VMEM((32, PART, 128), bf16),
            [pltpu.VMEM((count, PART, 128), bf16) for count in (248, 248, 248, 254)],
            [pltpu.VMEM((256, PART, 128), bf16)] * 4,
            [pltpu.VMEM((256, PART, 128), bf16)] * 4,
            [pltpu.VMEM((256, PART, 128), bf16)] * 4,
            pltpu.VMEM((32, 128, 256), bf16),
            pltpu.VMEM((32, 64, 128), f32),
            pltpu.VMEM((32, 64, 128), bf16),
            pltpu.VMEM((1, 128), i32),
            pltpu.VMEM((128, 128), i32),
            pltpu.VMEM((24, 128), i32),
            pltpu.SMEM((24, 128), i32),
            pltpu.VMEM((4, 128), i32),
            pltpu.SMEM((4, 128), i32),
            pltpu.VMEM((36, 10, 8, 128), bf16),
            pltpu.VMEM((36, 80, 128), f32),
            dma((9,)), dma((9,)), dma((13 + 3 * len(BATCHES),)), dma((2,)),
        ],
        compiler_params=pltpu.CompilerParams(
            collective_id=0, has_side_effects=True, vmem_limit_bytes=48 << 20
        ),
        name="block",
    )(*[pltpu.with_memory_space_constraint(x, pltpu.HBM) for x in operands])


def solution(mesh):
    in_specs = (P("rows", "cols", None), P("rows", "cols", None), P(), P(), P(), P(), P(), P(), P())
    out_specs = P("rows", "cols", None)
    return jax.shard_map(body, mesh=mesh, in_specs=in_specs, out_specs=out_specs, check_vma=False)
```

```python
import functools
import itertools
import math

import jax
import jax.numpy as jnp
from jax import lax
from jax.experimental import pallas as pl
from jax.experimental.pallas import tpu as pltpu
from jax.sharding import PartitionSpec as P

MESH = pl.DeviceIdType.MESH
HEADS = 4
EPSILON = 1e-06
BIG = 1 << 20


def hops(offset):
    return sum(min(step, 4 - step) for step in offset[1:])


OFFSETS = sorted(
    (o for o in itertools.product(range(2), range(4), range(4), range(4)) if any(o)), key=hops
)


PART = 16
PLANE = sorted(
    (o for o in itertools.product(range(2), range(4), range(4)) if any(o)), key=hops
)
BATCHES = (range(0, 8), range(8, 16), range(16, 22), range(22, 27), range(27, 31))
BATCH_OF = [b for b, members in enumerate(BATCHES) for _ in members]


def widened(part, offset):
    dc, first, second = offset
    return ((dc, first, second, 0), (dc, 0, second, first), (dc, first, 0, second))[part]


def layer_norm(floats, gain):
    centered = floats - jnp.mean(floats, axis=-1, keepdims=True)
    spread = jnp.mean(centered * centered, axis=-1, keepdims=True)
    return centered * lax.rsqrt(spread + EPSILON) * gain


def owner_of(route):
    return ((route >> 9) << 4) | ((route >> 3) & 15)


def local_of(route):
    return (((route >> 7) & 3) << 3) | (route & 7)


def to_strip(blocks):
    return blocks.reshape(8, 8, 8, 128).transpose(1, 0, 2, 3).reshape(8, 64, 128)


def block_kernel(
    image_hbm, routes_hbm, norm_gain_hbm, qkv_hbm, lce_hbm, out_w_hbm, mlp_gain_hbm, up_hbm, down_hbm,
    refined_ref,
    image_ref, routes_ref, norm_gain_ref, qkv_ref, lce_ref, out_w_ref, mlp_gain_ref, up_ref, down_ref,
    lines, straight, send, recv, keys_ref, values_ref, queries_ref, ctx_ref, combined,
    scores_ref, peaks_ref, expons_ref, totals_ref, weights_ref,
    my_routes, all_routes, slots, slots_smem, place, place_smem, grid_v, padded,
    load_sem, send_sem, recv_sem, local_sem,
):
    row, col = lax.axis_index("rows"), lax.axis_index("cols")
    chip_y, core = row // 2, row % 2
    chip_z, chip_x = col // 4, col % 4
    me = row * 16 + col
    spots = (chip_x, chip_y, chip_z)
    relays = (
        (core * 4 + chip_z) * 4 + chip_y,
        (core * 4 + chip_z) * 4 + chip_x,
        (core * 4 + chip_y) * 4 + chip_x,
    )
    over_last = (((1,), (1,)), ((), ()))
    over_first = (((0,), (0,)), ((), ()))

    def peer(offset):
        dc, dy, dz, dx = offset
        return (
            (chip_y + dy) % 4 * 2 + (core + dc) % 2,
            (chip_z + dz) % 4 * 4 + (chip_x + dx) % 4,
        )

    pairs = [
        (image_hbm, image_ref), (routes_hbm, routes_ref), (qkv_hbm, qkv_ref),
        (norm_gain_hbm, norm_gain_ref), (lce_hbm, lce_ref), (out_w_hbm, out_w_ref),
        (mlp_gain_hbm, mlp_gain_ref), (up_hbm, up_ref), (down_hbm, down_ref),
    ]
    loads = [pltpu.make_async_copy(a, b, load_sem.at[n]) for n, (a, b) in enumerate(pairs)]
    for load in loads:
        load.start()
    barrier = pltpu.get_barrier_semaphore()
    for offset in reversed(OFFSETS):
        pl.semaphore_signal(barrier, inc=1, device_id=peer(offset), device_id_type=MESH)
    for load in loads:
        load.wait()

    mine = jnp.concatenate(
        [routes_ref[i, t : t + 1, :] for i in range(4) for t in range(4)], axis=1
    )
    my_routes[...] = mine
    all_routes[pl.ds(me, 1), :] = mine

    gain = norm_gain_ref[...]
    for i in range(4):
        strip = image_ref[pl.ds(8 * i, 8)].astype(jnp.float32)
        strip = to_strip(layer_norm(strip, gain)).astype(jnp.bfloat16)
        for p in range(3):
            lines[p][spots[p], pl.ds(8 * i, 8)] = strip[:, PART * p : PART * p + PART]
        straight[pl.ds(8 * i, 8)] = strip[:, PART * 3 :]
        values = jnp.dot(
            strip.reshape(512, 128), qkv_ref[:, 256:384], preferred_element_type=jnp.float32
        )
        values = values.reshape(8, 8, 8, 128).transpose(1, 0, 2, 3)
        grid_v[pl.ds(2 + 8 * i, 8), pl.ds(1, 8)] = values.astype(jnp.bfloat16)

    lanes = lax.broadcasted_iota(jnp.int32, (128, 128), 1)
    subs = lax.broadcasted_iota(jnp.int32, (128, 128), 0)
    owners = jnp.broadcast_to(owner_of(mine), (128, 128))
    same = jnp.logical_and(owners == owners.T, subs < lanes)
    second = jnp.max(jnp.where(same, 1, 0), axis=0, keepdims=True)
    own = owner_of(mine)
    oy, oc, oz, ox = own >> 5, (own >> 4) & 1, (own >> 2) & 3, own & 3
    place[pl.ds(0, 1), :] = ((oc * 4 + oz) * 4 + oy) * 8 + ox * 2 + second
    place[pl.ds(1, 1), :] = ((oc * 4 + oz) * 4 + ox) * 8 + oy * 2 + second
    place[pl.ds(2, 1), :] = ((oc * 4 + oy) * 4 + ox) * 8 + oz * 2 + second
    place[pl.ds(3, 1), :] = own * 2 + second
    to_places = pltpu.make_async_copy(place, place_smem, local_sem.at[1])
    to_places.start()

    pl.semaphore_wait(barrier, len(OFFSETS))

    route_copies = []
    for n, offset in enumerate(OFFSETS[::-1]):
        route_copies.append(
            pltpu.make_async_remote_copy(
                src_ref=my_routes,
                dst_ref=all_routes.at[pl.ds(me, 1)],
                send_sem=send_sem.at[0],
                recv_sem=recv_sem.at[0],
                device_id=peer(offset),
                device_id_type=MESH,
            )
        )
        route_copies[-1].start()

    halo_copies = []
    for n, (dr, dc) in enumerate(
        (dr, dc) for dr in (-1, 0, 1) for dc in (-1, 0, 1) if (dr, dc) != (0, 0)
    ):
        rows = {-1: (2, 34, 2), 0: (2, 2, 32), 1: (32, 0, 2)}[dr]
        cols = {-1: (1, 9, 1), 0: (1, 1, 8), 1: (8, 0, 1)}[dc]
        halo_copies.append(
            pltpu.make_async_remote_copy(
                src_ref=grid_v.at[pl.ds(rows[0], rows[2]), pl.ds(cols[0], cols[2])],
                dst_ref=grid_v.at[pl.ds(rows[1], rows[2]), pl.ds(cols[1], cols[2])],
                send_sem=send_sem.at[1],
                recv_sem=recv_sem.at[1 + n],
                device_id=((row + dr + 8) % 8, (col + dc + 16) % 16),
                device_id_type=MESH,
            )
        )
        halo_copies[-1].start()

    line_copies = []
    for p in range(3):
        for step in (1, 3, 2):
            offset = tuple(step if axis == 3 - (0, 2, 1)[p] else 0 for axis in range(4))
            line_copies.append(
                pltpu.make_async_remote_copy(
                    src_ref=lines[p].at[spots[p]],
                    dst_ref=lines[p].at[spots[p]],
                    send_sem=send_sem.at[2 + p],
                    recv_sem=recv_sem.at[9 + p],
                    device_id=peer(offset),
                    device_id_type=MESH,
                )
            )
            line_copies[-1].start()

    query_w = qkv_ref[:, 0:128].T
    feature_head = lax.broadcasted_iota(jnp.int32, (128, 256), 0) // 32
    across_head = lax.broadcasted_iota(jnp.int32, (128, 256), 1) // 64
    own_head = feature_head == across_head

    def lay_out(r):
        tokens = jnp.concatenate(
            [lines[p][spots[p], r] for p in range(3)] + [straight[r]], axis=0
        )
        wide = lax.dot_general(
            query_w, jnp.concatenate([tokens] * 4, axis=0), over_last,
            preferred_element_type=jnp.float32,
        )
        queries_ref[r] = jnp.where(own_head, wide, 0.0).astype(jnp.bfloat16)

    @pl.loop(0, 8)
    def _(i):
        for j in range(4):
            lay_out(4 * i + j)

    def wait_bytes(ref, sem):
        pltpu.make_async_copy(ref, ref, sem).wait()

    wait_bytes(all_routes.at[pl.ds(0, 127)], recv_sem.at[0])

    table = all_routes[...].T
    order = subs * 32 + local_of(table)
    table_owner = owner_of(table)
    for p in range(3):
        for i in range(4):
            owner = (
                row * 16 + chip_z * 4 + i,
                (i * 2 + core) * 16 + col,
                row * 16 + i * 4 + chip_x,
            )[p]
            hits = table_owner == owner
            first = jnp.min(jnp.where(hits, order, BIG), axis=0, keepdims=True) & 31
            last = jnp.max(jnp.where(hits, order, 0), axis=0, keepdims=True) & 31
            slots[pl.ds(8 * p + 2 * i, 1), :] = first
            slots[pl.ds(8 * p + 2 * i + 1, 1), :] = last
    to_scalars = pltpu.make_async_copy(slots, slots_smem, local_sem.at[0])
    to_scalars.start()
    to_scalars.wait()

    def fill(p, number, into, base):
        for i in range(4):
            for t in range(2):
                into[base + 2 * i + t] = lines[p][i, slots_smem[8 * p + 2 * i + t, number]]

    def launch(p, n):
        pltpu.make_async_remote_copy(
            src_ref=send[p].at[pl.ds(8 * n, 8)],
            dst_ref=recv[p].at[pl.ds(8 * relays[p], 8)],
            send_sem=send_sem.at[5 + p],
            recv_sem=recv_sem.at[12 + len(BATCHES) * p + BATCH_OF[n]],
            device_id=peer(widened(p, PLANE[n])),
            device_id_type=MESH,
        ).start()

    def fill_straight(number, into, base):
        for t in range(2):
            into[base + t] = straight[slots_smem[2 * chip_x + t, number]]

    def launch_straight(n):
        pltpu.make_async_remote_copy(
            src_ref=send[3].at[pl.ds(2 * n, 2)],
            dst_ref=recv[3].at[pl.ds(2 * me, 2)],
            send_sem=send_sem.at[8],
            recv_sem=recv_sem.at[12 + 3 * len(BATCHES)],
            device_id=peer(OFFSETS[n]),
            device_id_type=MESH,
        ).start()

    pending = []

    def queue(start, *which):
        pending.append((start, which))
        if len(pending) > 2:
            begin, what = pending.pop(0)
            begin(*what)

    for n, offset in enumerate(OFFSETS):
        target = peer(offset)
        fill_straight(target[0] * 16 + target[1], send[3], 2 * n)
        queue(launch_straight, n)
    for p in range(3):
        wait_bytes(lines[p].at[pl.ds(0, 3)], recv_sem.at[9 + p])
    for n in range(31):
        for p in range(3):
            target = peer(widened(p, PLANE[n]))
            fill(p, target[0] * 16 + target[1], send[p], 8 * n)
            queue(launch, p, n)
    for p in range(3):
        fill(p, me, recv[p], 8 * relays[p])
    fill_straight(me, recv[3], 2 * me)
    for begin, what in pending:
        begin(*what)

    for copy in halo_copies:
        copy.wait_recv()
    keep_top, keep_bottom = row > 0, row < 7
    keep_left, keep_right = col > 0, col < 15

    @pl.loop(0, 36)
    def _(i):
        inside = jnp.logical_and(
            jnp.logical_or(i >= 2, keep_top), jnp.logical_or(i < 34, keep_bottom)
        )
        for j in range(10):
            keep = inside
            if j == 0:
                keep = jnp.logical_and(inside, keep_left)
            if j == 9:
                keep = jnp.logical_and(inside, keep_right)
            padded[i, pl.ds(8 * j, 8), :] = jnp.where(keep, grid_v[i, j].astype(jnp.float32), 0.0)

    @pl.loop(0, 8)
    def _(j):
        weights = [[lce_ref[a, pl.ds(b, 1), :] for b in range(5)] for a in range(5)]
        for i in range(4):
            totals = [None] * 8
            for line in range(12):
                for b in range(5):
                    window = padded[8 * i + line, pl.ds(8 * j + 6 + b, 8), :]
                    for a in range(5):
                        t = line - a
                        if 0 <= t < 8:
                            term = window * weights[a][b]
                            totals[t] = term if totals[t] is None else totals[t] + term
            for t in range(8):
                ctx_ref[8 * i + j, pl.ds(8 * t, 8), :] = totals[t]

    def project(p, first, count):
        tokens = recv[p][pl.ds(first, count)].reshape(count * PART, 128)
        both = jnp.dot(tokens, qkv_ref[:, 128:384], preferred_element_type=jnp.float32)
        both = both.astype(jnp.bfloat16)
        keys_ref[p][pl.ds(first, count)] = both[:, :128].reshape(count, PART, 128)
        values_ref[p][pl.ds(first, count)] = both[:, 128:].reshape(count, PART, 128)

    for p in range(3):
        project(p, 8 * relays[p], 8)
    wait_bytes(recv[3].at[pl.ds(0, 254)], recv_sem.at[12 + 3 * len(BATCHES)])

    @pl.loop(0, 16)
    def _(i):
        project(3, 16 * i, 16)

    for batch, p in itertools.product(range(len(BATCHES)), range(3)):
        members = BATCHES[batch]
        wait_bytes(
            recv[p].at[pl.ds(0, 8 * len(members))], recv_sem.at[12 + len(BATCHES) * p + batch]
        )
        for n in members:
            dc, first, second = PLANE[n]
            y, x, z = chip_y + 4, chip_x + 4, chip_z + 4
            low, high = ((y, z), (x, z), (x, y))[p]
            if p == 2:
                first, second = second, first
            relay = ((core + dc) % 2 * 4 + (high - second) % 4) * 4 + (low - first) % 4
            project(p, 8 * relay, 8)
    to_places.wait()

    factor = 32 ** (-0.5) / math.log(2)
    low_lanes = lax.broadcasted_iota(jnp.int32, (32, 128), 1) < 64

    def gather(parts, r):
        base = (r // 8) * 32 + r % 8
        return jnp.concatenate(
            [parts[p][place_smem[p, base + 8 * t]] for t in range(4) for p in range(4)], axis=0
        )

    def score(r, j):
        scores = jnp.dot(gather(keys_ref, r), queries_ref[r], preferred_element_type=jnp.float32)
        scores_ref[j][...] = scores
        peaks_ref[j][...] = jnp.max(scores, axis=0, keepdims=True)

    def soften(j):
        expons = jnp.exp2((scores_ref[j][...] - peaks_ref[j][...]) * factor)
        expons_ref[j][...] = expons
        totals_ref[j][...] = jnp.sum(expons, axis=0, keepdims=True)

    def weigh(j):
        scale = 1.0 / totals_ref[j][...]
        weights_ref[j][...] = (expons_ref[j][...] * scale).astype(jnp.bfloat16)

    def blend(r, j):
        blended = lax.dot_general(
            gather(values_ref, r), weights_ref[j][...], over_first,
            preferred_element_type=jnp.float32,
        )
        parts = []
        for h in range(HEADS):
            half = slice(128 * (h // 2), 128 * (h // 2) + 128)
            part = blended[32 * h : 32 * h + 32, half]
            parts.append(pltpu.roll(part, 64, 1) if h % 2 != j % 2 else part)
        return parts

    @pl.loop(0, 32 // GROUP + 3)
    def _(g):
        done = jnp.maximum(g - 3, 0) * GROUP
        for j in range(0, GROUP, 2):
            even, odd = blend(done + j, j), blend(done + j + 1, j + 1)
            both = jnp.concatenate([jnp.where(low_lanes, a, b) for a, b in zip(even, odd)], axis=0)
            attended = both.T.reshape(2, 64, 128) + ctx_ref[pl.ds(done + j, 2)]
            combined[pl.ds(done + j, 2)] = attended.astype(jnp.bfloat16)
        for j in range(GROUP):
            weigh(j)
        for j in range(GROUP):
            soften(j)
        ahead = jnp.minimum(g, 32 // GROUP - 1) * GROUP
        for j in range(GROUP):
            score(ahead + j, j)

    @pl.loop(0, 4)
    def _(i):
        strip = to_strip(image_ref[pl.ds(8 * i, 8)].astype(jnp.float32)).reshape(512, 128)
        mixed = jnp.dot(
            combined[pl.ds(8 * i, 8)].reshape(512, 128), out_w_ref[...],
            preferred_element_type=jnp.float32,
        )
        stored = (strip + mixed).astype(jnp.bfloat16).astype(jnp.float32)
        second = layer_norm(stored, mlp_gain_ref[...]).astype(jnp.bfloat16)
        lifted = jnp.dot(second, up_ref[...], preferred_element_type=jnp.float32)
        hidden = jax.nn.gelu(lifted, approximate=True).astype(jnp.bfloat16)
        lowered = jnp.dot(hidden, down_ref[...], preferred_element_type=jnp.float32)
        refined = (stored + lowered).reshape(8, 64, 128)
        refined_ref[pl.ds(8 * i, 8)] = to_strip(refined).astype(jnp.bfloat16)

    wait_bytes(all_routes.at[pl.ds(0, 127)], send_sem.at[0])
    for copy in halo_copies:
        wait_bytes(copy.src_ref, send_sem.at[1])
    for p in range(3):
        wait_bytes(lines[p].at[pl.ds(0, 3)], send_sem.at[2 + p])
        wait_bytes(send[p], send_sem.at[5 + p])
    wait_bytes(send[3], send_sem.at[8])


GROUP = 4


def body(
    image, routes, norm_gain, qkv_weight, lce_weight, out_weight, mlp_gain, up_weight, down_weight
):
    operands = (
        image, routes.transpose(0, 2, 1), norm_gain[None], qkv_weight, lce_weight, out_weight,
        mlp_gain[None], up_weight, down_weight,
    )
    hbm = pl.BlockSpec(memory_space=pltpu.HBM)
    dma = pltpu.SemaphoreType.DMA
    bf16, f32, i32 = jnp.bfloat16, jnp.float32, jnp.int32
    return pl.pallas_call(
        block_kernel,
        out_shape=jax.ShapeDtypeStruct((32, 64, 128), bf16),
        in_specs=[hbm] * 9,
        out_specs=pl.BlockSpec(memory_space=pltpu.VMEM),
        scratch_shapes=[pltpu.VMEM(x.shape, x.dtype) for x in operands] + [
            [pltpu.VMEM((4, 32, PART, 128), bf16)] * 3,
            pltpu.VMEM((32, PART, 128), bf16),
            [pltpu.VMEM((count, PART, 128), bf16) for count in (248, 248, 248, 254)],
            [pltpu.VMEM((256, PART, 128), bf16)] * 4,
            [pltpu.VMEM((256, PART, 128), bf16)] * 4,
            [pltpu.VMEM((256, PART, 128), bf16)] * 4,
            pltpu.VMEM((32, 128, 256), bf16),
            pltpu.VMEM((32, 64, 128), f32),
            pltpu.VMEM((32, 64, 128), bf16),
            [pltpu.VMEM((256, 256), f32)] * GROUP,
            [pltpu.VMEM((1, 256), f32)] * GROUP,
            [pltpu.VMEM((256, 256), f32)] * GROUP,
            [pltpu.VMEM((1, 256), f32)] * GROUP,
            [pltpu.VMEM((256, 256), bf16)] * GROUP,
            pltpu.VMEM((1, 128), i32),
            pltpu.VMEM((128, 128), i32),
            pltpu.VMEM((24, 128), i32),
            pltpu.SMEM((24, 128), i32),
            pltpu.VMEM((4, 128), i32),
            pltpu.SMEM((4, 128), i32),
            pltpu.VMEM((36, 10, 8, 128), bf16),
            pltpu.VMEM((36, 80, 128), f32),
            dma((9,)), dma((9,)), dma((13 + 3 * len(BATCHES),)), dma((2,)),
        ],
        compiler_params=pltpu.CompilerParams(
            collective_id=0, has_side_effects=True, vmem_limit_bytes=48 << 20
        ),
        name="block",
    )(*[pltpu.with_memory_space_constraint(x, pltpu.HBM) for x in operands])


def solution(mesh):
    in_specs = (P("rows", "cols", None), P("rows", "cols", None), P(), P(), P(), P(), P(), P(), P())
    out_specs = P("rows", "cols", None)
    return jax.shard_map(body, mesh=mesh, in_specs=in_specs, out_specs=out_specs, check_vma=False)
```

```python
import functools
import itertools
import math

import jax
import jax.numpy as jnp
from jax import lax
from jax.experimental import pallas as pl
from jax.experimental.pallas import tpu as pltpu
from jax.sharding import PartitionSpec as P

MESH = pl.DeviceIdType.MESH
HEADS = 4
EPSILON = 1e-06
BIG = 1 << 20


def hops(offset):
    return sum(min(step, 4 - step) for step in offset[1:])


OFFSETS = sorted(
    (o for o in itertools.product(range(2), range(4), range(4), range(4)) if any(o)), key=hops
)


PART = 16
PLANE = sorted(
    (o for o in itertools.product(range(2), range(4), range(4)) if any(o)), key=hops
)
BATCHES = (
    range(0, 8), range(8, 16), range(16, 22), range(22, 26), range(26, 29), range(29, 31)
)
BATCH_OF = [b for b, members in enumerate(BATCHES) for _ in members]


def widened(part, offset):
    dc, first, second = offset
    return ((dc, first, second, 0), (dc, 0, second, first), (dc, first, 0, second))[part]


def layer_norm(floats, gain):
    centered = floats - jnp.mean(floats, axis=-1, keepdims=True)
    spread = jnp.mean(centered * centered, axis=-1, keepdims=True)
    return centered * lax.rsqrt(spread + EPSILON) * gain


def owner_of(route):
    return ((route >> 9) << 4) | ((route >> 3) & 15)


def local_of(route):
    return (((route >> 7) & 3) << 3) | (route & 7)


def to_strip(blocks):
    return blocks.reshape(8, 8, 8, 128).transpose(1, 0, 2, 3).reshape(8, 64, 128)


def block_kernel(
    image_hbm, routes_hbm, norm_gain_hbm, qkv_hbm, lce_hbm, out_w_hbm, mlp_gain_hbm, up_hbm, down_hbm,
    refined_ref,
    image_ref, routes_ref, norm_gain_ref, qkv_ref, lce_ref, out_w_ref, mlp_gain_ref, up_ref, down_ref,
    lines, straight, send, recv, keys_ref, values_ref, queries_ref, ctx_ref, combined,
    scores_ref, peaks_ref, expons_ref, totals_ref, weights_ref,
    my_routes, all_routes, slots, slots_smem, place, place_smem, grid_v, padded, edge_rows, edge_send, edge_recv,
    load_sem, send_sem, recv_sem, local_sem,
):
    row, col = lax.axis_index("rows"), lax.axis_index("cols")
    chip_y, core = row // 2, row % 2
    chip_z, chip_x = col // 4, col % 4
    me = row * 16 + col
    spots = (chip_x, chip_y, chip_z)
    relays = (
        (core * 4 + chip_z) * 4 + chip_y,
        (core * 4 + chip_z) * 4 + chip_x,
        (core * 4 + chip_y) * 4 + chip_x,
    )
    over_last = (((1,), (1,)), ((), ()))
    over_first = (((0,), (0,)), ((), ()))

    def peer(offset):
        dc, dy, dz, dx = offset
        return (
            (chip_y + dy) % 4 * 2 + (core + dc) % 2,
            (chip_z + dz) % 4 * 4 + (chip_x + dx) % 4,
        )

    pairs = [
        (image_hbm, image_ref), (routes_hbm, routes_ref), (qkv_hbm, qkv_ref),
        (norm_gain_hbm, norm_gain_ref), (lce_hbm, lce_ref), (out_w_hbm, out_w_ref),
        (mlp_gain_hbm, mlp_gain_ref), (up_hbm, up_ref), (down_hbm, down_ref),
    ]
    loads = [pltpu.make_async_copy(a, b, load_sem.at[n]) for n, (a, b) in enumerate(pairs)]
    for load in loads:
        load.start()
    barrier = pltpu.get_barrier_semaphore()
    for offset in reversed(OFFSETS):
        pl.semaphore_signal(barrier, inc=1, device_id=peer(offset), device_id_type=MESH)
    for load in loads:
        load.wait()

    mine = jnp.concatenate(
        [routes_ref[i, t : t + 1, :] for i in range(4) for t in range(4)], axis=1
    )
    my_routes[...] = mine
    all_routes[pl.ds(me, 1), :] = mine

    gain = norm_gain_ref[...]
    for i in range(4):
        strip = image_ref[pl.ds(8 * i, 8)].astype(jnp.float32)
        strip = to_strip(layer_norm(strip, gain)).astype(jnp.bfloat16)
        for p in range(3):
            lines[p][spots[p], pl.ds(8 * i, 8)] = strip[:, PART * p : PART * p + PART]
        straight[pl.ds(8 * i, 8)] = strip[:, PART * 3 :]
        values = jnp.dot(
            strip.reshape(512, 128), qkv_ref[:, 256:384], preferred_element_type=jnp.float32
        )
        values = values.reshape(8, 8, 8, 128).transpose(1, 0, 2, 3)
        grid_v[pl.ds(2 + 8 * i, 8), pl.ds(1, 8)] = values.astype(jnp.bfloat16)
        for t in range(8):
            edge_rows[0, pl.ds(16 * i + 2 * t, 2), :] = values[t, 0, 0:2, :]
            edge_rows[1, pl.ds(16 * i + 2 * t, 2), :] = values[t, 7, 6:8, :]
    edge_send[...] = edge_rows[...].astype(jnp.bfloat16)

    lanes = lax.broadcasted_iota(jnp.int32, (128, 128), 1)
    subs = lax.broadcasted_iota(jnp.int32, (128, 128), 0)
    owners = jnp.broadcast_to(owner_of(mine), (128, 128))
    same = jnp.logical_and(owners == owners.T, subs < lanes)
    second = jnp.max(jnp.where(same, 1, 0), axis=0, keepdims=True)
    own = owner_of(mine)
    oy, oc, oz, ox = own >> 5, (own >> 4) & 1, (own >> 2) & 3, own & 3
    place[pl.ds(0, 1), :] = ((oc * 4 + oz) * 4 + oy) * 8 + ox * 2 + second
    place[pl.ds(1, 1), :] = ((oc * 4 + oz) * 4 + ox) * 8 + oy * 2 + second
    place[pl.ds(2, 1), :] = ((oc * 4 + oy) * 4 + ox) * 8 + oz * 2 + second
    place[pl.ds(3, 1), :] = own * 2 + second
    to_places = pltpu.make_async_copy(place, place_smem, local_sem.at[1])
    to_places.start()

    pl.semaphore_wait(barrier, len(OFFSETS))

    route_copies = []
    for n, offset in enumerate(OFFSETS[::-1]):
        route_copies.append(
            pltpu.make_async_remote_copy(
                src_ref=my_routes,
                dst_ref=all_routes.at[pl.ds(me, 1)],
                send_sem=send_sem.at[0],
                recv_sem=recv_sem.at[0],
                device_id=peer(offset),
                device_id_type=MESH,
            )
        )
        route_copies[-1].start()

    halo_copies = []
    for n, (dr, dc) in enumerate(
        (dr, dc) for dr in (-1, 0, 1) for dc in (-1, 0, 1) if (dr, dc) != (0, 0)
    ):
        if dr == 0:
            source, sink = edge_send.at[(dc + 1) // 2], edge_recv.at[(1 - dc) // 2]
        else:
            rows = {-1: (2, 34), 1: (32, 0)}[dr]
            cols = {-1: (1, 9, 1), 0: (1, 1, 8), 1: (8, 0, 1)}[dc]
            source = grid_v.at[pl.ds(rows[0], 2), pl.ds(cols[0], cols[2])]
            sink = grid_v.at[pl.ds(rows[1], 2), pl.ds(cols[1], cols[2])]
        halo_copies.append(
            pltpu.make_async_remote_copy(
                src_ref=source,
                dst_ref=sink,
                send_sem=send_sem.at[1],
                recv_sem=recv_sem.at[1 + n],
                device_id=((row + dr + 8) % 8, (col + dc + 16) % 16),
                device_id_type=MESH,
            )
        )
        halo_copies[-1].start()

    line_copies = []
    for p in range(3):
        for step in (1, 3, 2):
            offset = tuple(step if axis == 3 - (0, 2, 1)[p] else 0 for axis in range(4))
            line_copies.append(
                pltpu.make_async_remote_copy(
                    src_ref=lines[p].at[spots[p]],
                    dst_ref=lines[p].at[spots[p]],
                    send_sem=send_sem.at[2 + p],
                    recv_sem=recv_sem.at[9 + p],
                    device_id=peer(offset),
                    device_id_type=MESH,
                )
            )
            line_copies[-1].start()

    query_w = qkv_ref[:, 0:128].T
    feature_head = lax.broadcasted_iota(jnp.int32, (128, 256), 0) // 32
    across_head = lax.broadcasted_iota(jnp.int32, (128, 256), 1) // 64
    own_head = feature_head == across_head

    def lay_out(r):
        tokens = jnp.concatenate(
            [lines[p][spots[p], r] for p in range(3)] + [straight[r]], axis=0
        )
        wide = lax.dot_general(
            query_w, jnp.concatenate([tokens] * 4, axis=0), over_last,
            preferred_element_type=jnp.float32,
        )
        queries_ref[r] = jnp.where(own_head, wide, 0.0).astype(jnp.bfloat16)

    @pl.loop(0, 8)
    def _(i):
        for j in range(4):
            lay_out(4 * i + j)

    def wait_bytes(ref, sem):
        pltpu.make_async_copy(ref, ref, sem).wait()

    wait_bytes(all_routes.at[pl.ds(0, 127)], recv_sem.at[0])

    table = all_routes[...].T
    order = subs * 32 + local_of(table)
    table_owner = owner_of(table)
    for p in range(3):
        for i in range(4):
            owner = (
                row * 16 + chip_z * 4 + i,
                (i * 2 + core) * 16 + col,
                row * 16 + i * 4 + chip_x,
            )[p]
            hits = table_owner == owner
            first = jnp.min(jnp.where(hits, order, BIG), axis=0, keepdims=True) & 31
            last = jnp.max(jnp.where(hits, order, 0), axis=0, keepdims=True) & 31
            slots[pl.ds(8 * p + 2 * i, 1), :] = first
            slots[pl.ds(8 * p + 2 * i + 1, 1), :] = last
    to_scalars = pltpu.make_async_copy(slots, slots_smem, local_sem.at[0])
    to_scalars.start()
    to_scalars.wait()

    def fill(p, number, into, base):
        for i in range(4):
            for t in range(2):
                into[base + 2 * i + t] = lines[p][i, slots_smem[8 * p + 2 * i + t, number]]

    def launch(p, n):
        pltpu.make_async_remote_copy(
            src_ref=send[p].at[pl.ds(8 * n, 8)],
            dst_ref=recv[p].at[pl.ds(8 * relays[p], 8)],
            send_sem=send_sem.at[5 + p],
            recv_sem=recv_sem.at[12 + len(BATCHES) * p + BATCH_OF[n]],
            device_id=peer(widened(p, PLANE[n])),
            device_id_type=MESH,
        ).start()

    def fill_straight(number, into, base):
        for t in range(2):
            into[base + t] = straight[slots_smem[2 * chip_x + t, number]]

    def launch_straight(n):
        pltpu.make_async_remote_copy(
            src_ref=send[3].at[pl.ds(2 * n, 2)],
            dst_ref=recv[3].at[pl.ds(2 * me, 2)],
            send_sem=send_sem.at[8],
            recv_sem=recv_sem.at[12 + 3 * len(BATCHES)],
            device_id=peer(OFFSETS[n]),
            device_id_type=MESH,
        ).start()

    pending = []

    def queue(start, *which):
        pending.append((start, which))
        if len(pending) > 2:
            begin, what = pending.pop(0)
            begin(*what)

    for n, offset in enumerate(OFFSETS):
        target = peer(offset)
        fill_straight(target[0] * 16 + target[1], send[3], 2 * n)
        queue(launch_straight, n)
    for p in range(3):
        wait_bytes(lines[p].at[pl.ds(0, 3)], recv_sem.at[9 + p])
    for n in range(31):
        for p in range(3):
            target = peer(widened(p, PLANE[n]))
            fill(p, target[0] * 16 + target[1], send[p], 8 * n)
            queue(launch, p, n)
    for p in range(3):
        fill(p, me, recv[p], 8 * relays[p])
    fill_straight(me, recv[3], 2 * me)
    for begin, what in pending:
        begin(*what)

    for copy in halo_copies:
        copy.wait_recv()
    keep_top, keep_bottom = row > 0, row < 7
    keep_left, keep_right = col > 0, col < 15

    @pl.loop(0, 36)
    def _(i):
        inside = jnp.logical_and(
            jnp.logical_or(i >= 2, keep_top), jnp.logical_or(i < 34, keep_bottom)
        )
        for j in range(1, 9):
            padded[i, pl.ds(8 * j, 8), :] = jnp.where(inside, grid_v[i, j].astype(jnp.float32), 0.0)

    for j, keep in ((0, keep_left), (9, keep_right)):
        for i, also in ((0, keep_top), (1, keep_top), (34, keep_bottom), (35, keep_bottom)):
            padded[i, pl.ds(8 * j, 8), :] = jnp.where(
                jnp.logical_and(keep, also), grid_v[i, j].astype(jnp.float32), 0.0
            )
    for side, keep in ((0, keep_left), (1, keep_right)):
        edge_rows[side] = jnp.where(keep, edge_recv[side].astype(jnp.float32), 0.0)
        for i in range(32):
            padded[2 + i, pl.ds((6, 72)[side], 2), :] = edge_rows[side, pl.ds(2 * i, 2), :]

    @pl.loop(0, 8)
    def _(j):
        weights = [[lce_ref[a, pl.ds(b, 1), :] for b in range(5)] for a in range(5)]
        for i in range(4):
            totals = [None] * 8
            for line in range(12):
                for b in range(5):
                    window = padded[8 * i + line, pl.ds(8 * j + 6 + b, 8), :]
                    for a in range(5):
                        t = line - a
                        if 0 <= t < 8:
                            term = window * weights[a][b]
                            totals[t] = term if totals[t] is None else totals[t] + term
            for t in range(8):
                ctx_ref[8 * i + j, pl.ds(8 * t, 8), :] = totals[t]

    def project(p, first, count):
        tokens = recv[p][pl.ds(first, count)].reshape(count * PART, 128)
        both = jnp.dot(tokens, qkv_ref[:, 128:384], preferred_element_type=jnp.float32)
        both = both.astype(jnp.bfloat16)
        keys_ref[p][pl.ds(first, count)] = both[:, :128].reshape(count, PART, 128)
        values_ref[p][pl.ds(first, count)] = both[:, 128:].reshape(count, PART, 128)

    for p in range(3):
        project(p, 8 * relays[p], 8)
    wait_bytes(recv[3].at[pl.ds(0, 254)], recv_sem.at[12 + 3 * len(BATCHES)])

    @pl.loop(0, 16)
    def _(i):
        project(3, 16 * i, 16)

    for batch, p in itertools.product(range(len(BATCHES)), range(3)):
        members = BATCHES[batch]
        wait_bytes(
            recv[p].at[pl.ds(0, 8 * len(members))], recv_sem.at[12 + len(BATCHES) * p + batch]
        )
        for n in members:
            dc, first, second = PLANE[n]
            y, x, z = chip_y + 4, chip_x + 4, chip_z + 4
            low, high = ((y, z), (x, z), (x, y))[p]
            if p == 2:
                first, second = second, first
            relay = ((core + dc) % 2 * 4 + (high - second) % 4) * 4 + (low - first) % 4
            project(p, 8 * relay, 8)
    to_places.wait()

    factor = 32 ** (-0.5) / math.log(2)
    low_lanes = lax.broadcasted_iota(jnp.int32, (32, 128), 1) < 64

    def gather(parts, r):
        base = (r // 8) * 32 + r % 8
        return jnp.concatenate(
            [parts[p][place_smem[p, base + 8 * t]] for t in range(4) for p in range(4)], axis=0
        )

    def score(r, j):
        scores = jnp.dot(gather(keys_ref, r), queries_ref[r], preferred_element_type=jnp.float32)
        scores_ref[j][...] = scores
        peaks_ref[j][...] = jnp.max(scores, axis=0, keepdims=True)

    def soften(j):
        expons = jnp.exp2((scores_ref[j][...] - peaks_ref[j][...]) * factor)
        expons_ref[j][...] = expons
        totals_ref[j][...] = jnp.sum(expons, axis=0, keepdims=True)

    def weigh(j):
        scale = 1.0 / totals_ref[j][...]
        weights_ref[j][...] = (expons_ref[j][...] * scale).astype(jnp.bfloat16)

    def blend(r, j):
        blended = lax.dot_general(
            gather(values_ref, r), weights_ref[j][...], over_first,
            preferred_element_type=jnp.float32,
        )
        parts = []
        for h in range(HEADS):
            half = slice(128 * (h // 2), 128 * (h // 2) + 128)
            part = blended[32 * h : 32 * h + 32, half]
            parts.append(pltpu.roll(part, 64, 1) if h % 2 != j % 2 else part)
        return parts

    def step(g):
        if g >= 3:
            done = (g - 3) * GROUP
            for j in range(0, GROUP, 2):
                even, odd = blend(done + j, j), blend(done + j + 1, j + 1)
                both = jnp.concatenate(
                    [jnp.where(low_lanes, a, b) for a, b in zip(even, odd)], axis=0
                )
                attended = both.T.reshape(2, 64, 128) + ctx_ref[pl.ds(done + j, 2)]
                combined[pl.ds(done + j, 2)] = attended.astype(jnp.bfloat16)
        if 2 <= g < STEPS + 2:
            for j in range(GROUP):
                weigh(j)
        if 1 <= g < STEPS + 1:
            for j in range(GROUP):
                soften(j)
        if g < STEPS:
            for j in range(GROUP):
                score(g * GROUP + j, j)

    for g in range(STEPS + 3):
        step(g)

    def finish(i):
        strip = to_strip(image_ref[pl.ds(8 * i, 8)].astype(jnp.float32)).reshape(512, 128)
        mixed = jnp.dot(
            combined[pl.ds(8 * i, 8)].reshape(512, 128), out_w_ref[...],
            preferred_element_type=jnp.float32,
        )
        stored = (strip + mixed).astype(jnp.bfloat16).astype(jnp.float32)
        second = layer_norm(stored, mlp_gain_ref[...]).astype(jnp.bfloat16)
        lifted = jnp.dot(second, up_ref[...], preferred_element_type=jnp.float32)
        hidden = jax.nn.gelu(lifted, approximate=True).astype(jnp.bfloat16)
        lowered = jnp.dot(hidden, down_ref[...], preferred_element_type=jnp.float32)
        refined = (stored + lowered).reshape(8, 64, 128)
        refined_ref[pl.ds(8 * i, 8)] = to_strip(refined).astype(jnp.bfloat16)

    for i in range(4):
        finish(i)

    wait_bytes(all_routes.at[pl.ds(0, 127)], send_sem.at[0])
    for copy in halo_copies:
        wait_bytes(copy.src_ref, send_sem.at[1])
    for p in range(3):
        wait_bytes(lines[p].at[pl.ds(0, 3)], send_sem.at[2 + p])
        wait_bytes(send[p], send_sem.at[5 + p])
    wait_bytes(send[3], send_sem.at[8])


GROUP = 4
STEPS = 32 // GROUP


def body(
    image, routes, norm_gain, qkv_weight, lce_weight, out_weight, mlp_gain, up_weight, down_weight
):
    operands = (
        image, routes.transpose(0, 2, 1), norm_gain[None], qkv_weight, lce_weight, out_weight,
        mlp_gain[None], up_weight, down_weight,
    )
    hbm = pl.BlockSpec(memory_space=pltpu.HBM)
    dma = pltpu.SemaphoreType.DMA
    bf16, f32, i32 = jnp.bfloat16, jnp.float32, jnp.int32
    return pl.pallas_call(
        block_kernel,
        out_shape=jax.ShapeDtypeStruct((32, 64, 128), bf16),
        in_specs=[hbm] * 9,
        out_specs=pl.BlockSpec(memory_space=pltpu.VMEM),
        scratch_shapes=[pltpu.VMEM(x.shape, x.dtype) for x in operands] + [
            [pltpu.VMEM((4, 32, PART, 128), bf16)] * 3,
            pltpu.VMEM((32, PART, 128), bf16),
            [pltpu.VMEM((count, PART, 128), bf16) for count in (248, 248, 248, 254)],
            [pltpu.VMEM((256, PART, 128), bf16)] * 4,
            [pltpu.VMEM((256, PART, 128), bf16)] * 4,
            [pltpu.VMEM((256, PART, 128), bf16)] * 4,
            pltpu.VMEM((32, 128, 256), bf16),
            pltpu.VMEM((32, 64, 128), f32),
            pltpu.VMEM((32, 64, 128), bf16),
            [pltpu.VMEM((256, 256), f32)] * GROUP,
            [pltpu.VMEM((1, 256), f32)] * GROUP,
            [pltpu.VMEM((256, 256), f32)] * GROUP,
            [pltpu.VMEM((1, 256), f32)] * GROUP,
            [pltpu.VMEM((256, 256), bf16)] * GROUP,
            pltpu.VMEM((1, 128), i32),
            pltpu.VMEM((128, 128), i32),
            pltpu.VMEM((24, 128), i32),
            pltpu.SMEM((24, 128), i32),
            pltpu.VMEM((4, 128), i32),
            pltpu.SMEM((4, 128), i32),
            pltpu.VMEM((36, 10, 8, 128), bf16),
            pltpu.VMEM((36, 80, 128), f32),
            pltpu.VMEM((2, 64, 128), f32),
            pltpu.VMEM((2, 64, 128), bf16),
            pltpu.VMEM((2, 64, 128), bf16),
            dma((9,)), dma((9,)), dma((13 + 3 * len(BATCHES),)), dma((2,)),
        ],
        compiler_params=pltpu.CompilerParams(
            collective_id=0, has_side_effects=True, vmem_limit_bytes=48 << 20
        ),
        name="block",
    )(*[pltpu.with_memory_space_constraint(x, pltpu.HBM) for x in operands])


def solution(mesh):
    in_specs = (P("rows", "cols", None), P("rows", "cols", None), P(), P(), P(), P(), P(), P(), P())
    out_specs = P("rows", "cols", None)
    return jax.shard_map(body, mesh=mesh, in_specs=in_specs, out_specs=out_specs, check_vma=False)
```

```python
import functools
import itertools
import math

import jax
import jax.numpy as jnp
from jax import lax
from jax.experimental import pallas as pl
from jax.experimental.pallas import tpu as pltpu
from jax.sharding import PartitionSpec as P

MESH = pl.DeviceIdType.MESH
HEADS = 4
EPSILON = 1e-06
BIG = 1 << 20


def hops(offset):
    return sum(min(step, 4 - step) for step in offset[1:])


OFFSETS = sorted(
    (o for o in itertools.product(range(2), range(4), range(4), range(4)) if any(o)), key=hops
)


PART = 16
PLANE = sorted(
    (o for o in itertools.product(range(2), range(4), range(4)) if any(o)), key=hops
)
BATCHES = (
    range(0, 8), range(8, 16), range(16, 22), range(22, 26), range(26, 29), range(29, 31)
)
BATCH_OF = [b for b, members in enumerate(BATCHES) for _ in members]


def widened(part, offset):
    dc, first, second = offset
    return ((dc, first, second, 0), (dc, 0, second, first), (dc, first, 0, second))[part]


def layer_norm(floats, gain):
    centered = floats - jnp.mean(floats, axis=-1, keepdims=True)
    spread = jnp.mean(centered * centered, axis=-1, keepdims=True)
    return centered * lax.rsqrt(spread + EPSILON) * gain


def owner_of(route):
    return ((route >> 9) << 4) | ((route >> 3) & 15)


def local_of(route):
    return (((route >> 7) & 3) << 3) | (route & 7)


def to_strip(blocks):
    return blocks.reshape(8, 8, 8, 128).transpose(1, 0, 2, 3).reshape(8, 64, 128)


def block_kernel(
    image_hbm, routes_hbm, norm_gain_hbm, qkv_hbm, lce_hbm, out_w_hbm, mlp_gain_hbm, up_hbm, down_hbm,
    refined_ref,
    image_ref, routes_ref, norm_gain_ref, qkv_ref, lce_ref, out_w_ref, mlp_gain_ref, up_ref, down_ref,
    lines, straight, send, recv, keys_ref, values_ref, queries_ref, ctx_ref, combined,
    scores_ref, peaks_ref, expons_ref, totals_ref, weights_ref,
    my_routes, all_routes, slots, slots_smem, place, place_smem, grid_v, padded, edge_rows, edge_send, edge_recv,
    load_sem, send_sem, recv_sem, local_sem,
):
    row, col = lax.axis_index("rows"), lax.axis_index("cols")
    chip_y, core = row // 2, row % 2
    chip_z, chip_x = col // 4, col % 4
    me = row * 16 + col
    spots = (chip_x, chip_y, chip_z)
    relays = (
        (core * 4 + chip_z) * 4 + chip_y,
        (core * 4 + chip_z) * 4 + chip_x,
        (core * 4 + chip_y) * 4 + chip_x,
    )
    over_last = (((1,), (1,)), ((), ()))
    over_first = (((0,), (0,)), ((), ()))

    def peer(offset):
        dc, dy, dz, dx = offset
        return (
            (chip_y + dy) % 4 * 2 + (core + dc) % 2,
            (chip_z + dz) % 4 * 4 + (chip_x + dx) % 4,
        )

    pairs = [
        (image_hbm, image_ref), (routes_hbm, routes_ref), (qkv_hbm, qkv_ref),
        (norm_gain_hbm, norm_gain_ref), (lce_hbm, lce_ref), (out_w_hbm, out_w_ref),
        (mlp_gain_hbm, mlp_gain_ref), (up_hbm, up_ref), (down_hbm, down_ref),
    ]
    loads = [pltpu.make_async_copy(a, b, load_sem.at[n]) for n, (a, b) in enumerate(pairs)]
    for load in loads:
        load.start()
    barrier = pltpu.get_barrier_semaphore()
    for offset in reversed(OFFSETS):
        pl.semaphore_signal(barrier, inc=1, device_id=peer(offset), device_id_type=MESH)
    for load in loads:
        load.wait()

    mine = jnp.concatenate(
        [routes_ref[i, t : t + 1, :] for i in range(4) for t in range(4)], axis=1
    )
    my_routes[...] = mine
    all_routes[pl.ds(me, 1), :] = mine

    gain = norm_gain_ref[...]
    for i in range(4):
        strip = image_ref[pl.ds(8 * i, 8)].astype(jnp.float32)
        strip = to_strip(layer_norm(strip, gain)).astype(jnp.bfloat16)
        for p in range(3):
            lines[p][spots[p], pl.ds(8 * i, 8)] = strip[:, PART * p : PART * p + PART]
        straight[pl.ds(8 * i, 8)] = strip[:, PART * 3 :]
        values = jnp.dot(
            strip.reshape(512, 128), qkv_ref[:, 256:384], preferred_element_type=jnp.float32
        )
        values = values.reshape(8, 8, 8, 128).transpose(1, 0, 2, 3)
        grid_v[pl.ds(2 + 8 * i, 8), pl.ds(1, 8)] = values.astype(jnp.bfloat16)
        for t in range(8):
            edge_rows[0, pl.ds(16 * i + 2 * t, 2), :] = values[t, 0, 0:2, :]
            edge_rows[1, pl.ds(16 * i + 2 * t, 2), :] = values[t, 7, 6:8, :]
    edge_send[...] = edge_rows[...].astype(jnp.bfloat16)

    lanes = lax.broadcasted_iota(jnp.int32, (128, 128), 1)
    subs = lax.broadcasted_iota(jnp.int32, (128, 128), 0)
    owners = jnp.broadcast_to(owner_of(mine), (128, 128))
    same = jnp.logical_and(owners == owners.T, subs < lanes)
    second = jnp.max(jnp.where(same, 1, 0), axis=0, keepdims=True)
    own = owner_of(mine)
    oy, oc, oz, ox = own >> 5, (own >> 4) & 1, (own >> 2) & 3, own & 3
    place[pl.ds(0, 1), :] = ((oc * 4 + oz) * 4 + oy) * 8 + ox * 2 + second
    place[pl.ds(1, 1), :] = ((oc * 4 + oz) * 4 + ox) * 8 + oy * 2 + second
    place[pl.ds(2, 1), :] = ((oc * 4 + oy) * 4 + ox) * 8 + oz * 2 + second
    place[pl.ds(3, 1), :] = own * 2 + second
    to_places = pltpu.make_async_copy(place, place_smem, local_sem.at[1])
    to_places.start()

    pl.semaphore_wait(barrier, len(OFFSETS))

    route_copies = []
    for n, offset in enumerate(OFFSETS[::-1]):
        route_copies.append(
            pltpu.make_async_remote_copy(
                src_ref=my_routes,
                dst_ref=all_routes.at[pl.ds(me, 1)],
                send_sem=send_sem.at[0],
                recv_sem=recv_sem.at[0],
                device_id=peer(offset),
                device_id_type=MESH,
            )
        )
        route_copies[-1].start()

    line_copies = []
    for p in range(3):
        for step in (2, 1, 3):
            offset = tuple(step if axis == 3 - (0, 2, 1)[p] else 0 for axis in range(4))
            line_copies.append(
                pltpu.make_async_remote_copy(
                    src_ref=lines[p].at[spots[p]],
                    dst_ref=lines[p].at[spots[p]],
                    send_sem=send_sem.at[2 + p],
                    recv_sem=recv_sem.at[9 + p],
                    device_id=peer(offset),
                    device_id_type=MESH,
                )
            )
            line_copies[-1].start()

    halo_copies = []
    for n, (dr, dc) in enumerate(
        (dr, dc) for dr in (-1, 0, 1) for dc in (-1, 0, 1) if (dr, dc) != (0, 0)
    ):
        if dr == 0:
            source, sink = edge_send.at[(dc + 1) // 2], edge_recv.at[(1 - dc) // 2]
        else:
            rows = {-1: (2, 34), 1: (32, 0)}[dr]
            cols = {-1: (1, 9, 1), 0: (1, 1, 8), 1: (8, 0, 1)}[dc]
            source = grid_v.at[pl.ds(rows[0], 2), pl.ds(cols[0], cols[2])]
            sink = grid_v.at[pl.ds(rows[1], 2), pl.ds(cols[1], cols[2])]
        halo_copies.append(
            pltpu.make_async_remote_copy(
                src_ref=source,
                dst_ref=sink,
                send_sem=send_sem.at[1],
                recv_sem=recv_sem.at[1 + n],
                device_id=((row + dr + 8) % 8, (col + dc + 16) % 16),
                device_id_type=MESH,
            )
        )
        halo_copies[-1].start()

    query_w = qkv_ref[:, 0:128].T
    feature_head = lax.broadcasted_iota(jnp.int32, (128, 256), 0) // 32
    across_head = lax.broadcasted_iota(jnp.int32, (128, 256), 1) // 64
    own_head = feature_head == across_head

    def lay_out(r):
        tokens = jnp.concatenate(
            [lines[p][spots[p], r] for p in range(3)] + [straight[r]], axis=0
        )
        wide = lax.dot_general(
            query_w, jnp.concatenate([tokens] * 4, axis=0), over_last,
            preferred_element_type=jnp.float32,
        )
        queries_ref[r] = jnp.where(own_head, wide, 0.0).astype(jnp.bfloat16)

    @pl.loop(0, 8)
    def _(i):
        for j in range(4):
            lay_out(4 * i + j)

    def wait_bytes(ref, sem):
        pltpu.make_async_copy(ref, ref, sem).wait()

    wait_bytes(all_routes.at[pl.ds(0, 127)], recv_sem.at[0])

    table = all_routes[...].T
    order = subs * 32 + local_of(table)
    table_owner = owner_of(table)
    for p in range(3):
        for i in range(4):
            owner = (
                row * 16 + chip_z * 4 + i,
                (i * 2 + core) * 16 + col,
                row * 16 + i * 4 + chip_x,
            )[p]
            hits = table_owner == owner
            first = jnp.min(jnp.where(hits, order, BIG), axis=0, keepdims=True) & 31
            last = jnp.max(jnp.where(hits, order, 0), axis=0, keepdims=True) & 31
            slots[pl.ds(8 * p + 2 * i, 1), :] = first
            slots[pl.ds(8 * p + 2 * i + 1, 1), :] = last
    to_scalars = pltpu.make_async_copy(slots, slots_smem, local_sem.at[0])
    to_scalars.start()
    to_scalars.wait()

    def fill(p, number, into, base):
        for i in range(4):
            for t in range(2):
                into[base + 2 * i + t] = lines[p][i, slots_smem[8 * p + 2 * i + t, number]]

    def launch(p, n):
        pltpu.make_async_remote_copy(
            src_ref=send[p].at[pl.ds(8 * n, 8)],
            dst_ref=recv[p].at[pl.ds(8 * relays[p], 8)],
            send_sem=send_sem.at[5 + p],
            recv_sem=recv_sem.at[12 + len(BATCHES) * p + BATCH_OF[n]],
            device_id=peer(widened(p, PLANE[n])),
            device_id_type=MESH,
        ).start()

    def fill_straight(number, into, base):
        for t in range(2):
            into[base + t] = straight[slots_smem[2 * chip_x + t, number]]

    def launch_straight(n):
        pltpu.make_async_remote_copy(
            src_ref=send[3].at[pl.ds(2 * n, 2)],
            dst_ref=recv[3].at[pl.ds(2 * me, 2)],
            send_sem=send_sem.at[8],
            recv_sem=recv_sem.at[12 + 3 * len(BATCHES)],
            device_id=peer(OFFSETS[n]),
            device_id_type=MESH,
        ).start()

    pending = []

    def queue(start, *which):
        pending.append((start, which))
        if len(pending) > 2:
            begin, what = pending.pop(0)
            begin(*what)

    for n, offset in enumerate(OFFSETS):
        target = peer(offset)
        fill_straight(target[0] * 16 + target[1], send[3], 2 * n)
        queue(launch_straight, n)
    for p in range(3):
        wait_bytes(lines[p].at[pl.ds(0, 3)], recv_sem.at[9 + p])
    for n in range(31):
        for p in range(3):
            target = peer(widened(p, PLANE[n]))
            fill(p, target[0] * 16 + target[1], send[p], 8 * n)
            queue(launch, p, n)
    for p in range(3):
        fill(p, me, recv[p], 8 * relays[p])
    fill_straight(me, recv[3], 2 * me)
    for begin, what in pending:
        begin(*what)

    for copy in halo_copies:
        copy.wait_recv()
    keep_top, keep_bottom = row > 0, row < 7
    keep_left, keep_right = col > 0, col < 15

    @pl.loop(0, 36)
    def _(i):
        inside = jnp.logical_and(
            jnp.logical_or(i >= 2, keep_top), jnp.logical_or(i < 34, keep_bottom)
        )
        for j in range(1, 9):
            padded[i, pl.ds(8 * j, 8), :] = jnp.where(inside, grid_v[i, j].astype(jnp.float32), 0.0)

    for j, keep in ((0, keep_left), (9, keep_right)):
        for i, also in ((0, keep_top), (1, keep_top), (34, keep_bottom), (35, keep_bottom)):
            padded[i, pl.ds(8 * j, 8), :] = jnp.where(
                jnp.logical_and(keep, also), grid_v[i, j].astype(jnp.float32), 0.0
            )
    for side, keep in ((0, keep_left), (1, keep_right)):
        edge_rows[side] = jnp.where(keep, edge_recv[side].astype(jnp.float32), 0.0)
        for i in range(32):
            padded[2 + i, pl.ds((6, 72)[side], 2), :] = edge_rows[side, pl.ds(2 * i, 2), :]

    @pl.loop(0, 8)
    def _(j):
        weights = [[lce_ref[a, pl.ds(b, 1), :] for b in range(5)] for a in range(5)]
        for i in range(4):
            totals = [None] * 8
            for line in range(12):
                for b in range(5):
                    window = padded[8 * i + line, pl.ds(8 * j + 6 + b, 8), :]
                    for a in range(5):
                        t = line - a
                        if 0 <= t < 8:
                            term = window * weights[a][b]
                            totals[t] = term if totals[t] is None else totals[t] + term
            for t in range(8):
                ctx_ref[8 * i + j, pl.ds(8 * t, 8), :] = totals[t]

    def project(p, first, count):
        tokens = recv[p][pl.ds(first, count)].reshape(count * PART, 128)
        both = jnp.dot(tokens, qkv_ref[:, 128:384], preferred_element_type=jnp.float32)
        both = both.astype(jnp.bfloat16)
        keys_ref[p][pl.ds(first, count)] = both[:, :128].reshape(count, PART, 128)
        values_ref[p][pl.ds(first, count)] = both[:, 128:].reshape(count, PART, 128)

    for p in range(3):
        project(p, 8 * relays[p], 8)
    wait_bytes(recv[3].at[pl.ds(0, 254)], recv_sem.at[12 + 3 * len(BATCHES)])

    @pl.loop(0, 16)
    def _(i):
        project(3, 16 * i, 16)

    for batch, p in itertools.product(range(len(BATCHES)), range(3)):
        members = BATCHES[batch]
        wait_bytes(
            recv[p].at[pl.ds(0, 8 * len(members))], recv_sem.at[12 + len(BATCHES) * p + batch]
        )
        for n in members:
            dc, first, second = PLANE[n]
            y, x, z = chip_y + 4, chip_x + 4, chip_z + 4
            low, high = ((y, z), (x, z), (x, y))[p]
            if p == 2:
                first, second = second, first
            relay = ((core + dc) % 2 * 4 + (high - second) % 4) * 4 + (low - first) % 4
            project(p, 8 * relay, 8)
    to_places.wait()

    factor = 32 ** (-0.5) / math.log(2)
    low_lanes = lax.broadcasted_iota(jnp.int32, (32, 128), 1) < 64

    def gather(parts, r):
        base = (r // 8) * 32 + r % 8
        return jnp.concatenate(
            [parts[p][place_smem[p, base + 8 * t]] for t in range(4) for p in range(4)], axis=0
        )

    def score(r, j):
        scores = jnp.dot(gather(keys_ref, r), queries_ref[r], preferred_element_type=jnp.float32)
        scores_ref[j][...] = scores
        peaks_ref[j][...] = jnp.max(scores, axis=0, keepdims=True)

    def soften(j):
        expons = jnp.exp2((scores_ref[j][...] - peaks_ref[j][...]) * factor)
        expons_ref[j][...] = expons
        totals_ref[j][...] = jnp.sum(expons, axis=0, keepdims=True)

    def weigh(j):
        scale = 1.0 / totals_ref[j][...]
        weights_ref[j][...] = (expons_ref[j][...] * scale).astype(jnp.bfloat16)

    def blend(r, j):
        blended = lax.dot_general(
            gather(values_ref, r), weights_ref[j][...], over_first,
            preferred_element_type=jnp.float32,
        )
        parts = []
        for h in range(HEADS):
            half = slice(128 * (h // 2), 128 * (h // 2) + 128)
            part = blended[32 * h : 32 * h + 32, half]
            parts.append(pltpu.roll(part, 64, 1) if h % 2 != j % 2 else part)
        return parts

    def step(g):
        if g >= 3:
            done = (g - 3) * GROUP
            for j in range(0, GROUP, 2):
                even, odd = blend(done + j, j), blend(done + j + 1, j + 1)
                both = jnp.concatenate(
                    [jnp.where(low_lanes, a, b) for a, b in zip(even, odd)], axis=0
                )
                attended = both.T.reshape(2, 64, 128) + ctx_ref[pl.ds(done + j, 2)]
                combined[pl.ds(done + j, 2)] = attended.astype(jnp.bfloat16)
        if 2 <= g < STEPS + 2:
            for j in range(GROUP):
                weigh(j)
        if 1 <= g < STEPS + 1:
            for j in range(GROUP):
                soften(j)
        if g < STEPS:
            for j in range(GROUP):
                score(g * GROUP + j, j)

    for g in range(STEPS + 3):
        step(g)

    def finish(i):
        strip = to_strip(image_ref[pl.ds(8 * i, 8)].astype(jnp.float32)).reshape(512, 128)
        mixed = jnp.dot(
            combined[pl.ds(8 * i, 8)].reshape(512, 128), out_w_ref[...],
            preferred_element_type=jnp.float32,
        )
        stored = (strip + mixed).astype(jnp.bfloat16).astype(jnp.float32)
        second = layer_norm(stored, mlp_gain_ref[...]).astype(jnp.bfloat16)
        lifted = jnp.dot(second, up_ref[...], preferred_element_type=jnp.float32)
        hidden = jax.nn.gelu(lifted, approximate=True).astype(jnp.bfloat16)
        lowered = jnp.dot(hidden, down_ref[...], preferred_element_type=jnp.float32)
        refined = (stored + lowered).reshape(8, 64, 128)
        refined_ref[pl.ds(8 * i, 8)] = to_strip(refined).astype(jnp.bfloat16)

    for i in range(4):
        finish(i)

    wait_bytes(all_routes.at[pl.ds(0, 127)], send_sem.at[0])
    for copy in halo_copies:
        wait_bytes(copy.src_ref, send_sem.at[1])
    for p in range(3):
        wait_bytes(lines[p].at[pl.ds(0, 3)], send_sem.at[2 + p])
        wait_bytes(send[p], send_sem.at[5 + p])
    wait_bytes(send[3], send_sem.at[8])


GROUP = 4
STEPS = 32 // GROUP


def body(
    image, routes, norm_gain, qkv_weight, lce_weight, out_weight, mlp_gain, up_weight, down_weight
):
    operands = (
        image, routes.transpose(0, 2, 1), norm_gain[None], qkv_weight, lce_weight, out_weight,
        mlp_gain[None], up_weight, down_weight,
    )
    hbm = pl.BlockSpec(memory_space=pltpu.HBM)
    dma = pltpu.SemaphoreType.DMA
    bf16, f32, i32 = jnp.bfloat16, jnp.float32, jnp.int32
    return pl.pallas_call(
        block_kernel,
        out_shape=jax.ShapeDtypeStruct((32, 64, 128), bf16),
        in_specs=[hbm] * 9,
        out_specs=pl.BlockSpec(memory_space=pltpu.VMEM),
        scratch_shapes=[pltpu.VMEM(x.shape, x.dtype) for x in operands] + [
            [pltpu.VMEM((4, 32, PART, 128), bf16)] * 3,
            pltpu.VMEM((32, PART, 128), bf16),
            [pltpu.VMEM((count, PART, 128), bf16) for count in (248, 248, 248, 254)],
            [pltpu.VMEM((256, PART, 128), bf16)] * 4,
            [pltpu.VMEM((256, PART, 128), bf16)] * 4,
            [pltpu.VMEM((256, PART, 128), bf16)] * 4,
            pltpu.VMEM((32, 128, 256), bf16),
            pltpu.VMEM((32, 64, 128), f32),
            pltpu.VMEM((32, 64, 128), bf16),
            [pltpu.VMEM((256, 256), f32)] * GROUP,
            [pltpu.VMEM((1, 256), f32)] * GROUP,
            [pltpu.VMEM((256, 256), f32)] * GROUP,
            [pltpu.VMEM((1, 256), f32)] * GROUP,
            [pltpu.VMEM((256, 256), bf16)] * GROUP,
            pltpu.VMEM((1, 128), i32),
            pltpu.VMEM((128, 128), i32),
            pltpu.VMEM((24, 128), i32),
            pltpu.SMEM((24, 128), i32),
            pltpu.VMEM((4, 128), i32),
            pltpu.SMEM((4, 128), i32),
            pltpu.VMEM((36, 10, 8, 128), bf16),
            pltpu.VMEM((36, 80, 128), f32),
            pltpu.VMEM((2, 64, 128), f32),
            pltpu.VMEM((2, 64, 128), bf16),
            pltpu.VMEM((2, 64, 128), bf16),
            dma((9,)), dma((9,)), dma((13 + 3 * len(BATCHES),)), dma((2,)),
        ],
        compiler_params=pltpu.CompilerParams(
            collective_id=0, has_side_effects=True, vmem_limit_bytes=48 << 20
        ),
        name="block",
    )(*[pltpu.with_memory_space_constraint(x, pltpu.HBM) for x in operands])


def solution(mesh):
    in_specs = (P("rows", "cols", None), P("rows", "cols", None), P(), P(), P(), P(), P(), P(), P())
    out_specs = P("rows", "cols", None)
    return jax.shard_map(body, mesh=mesh, in_specs=in_specs, out_specs=out_specs, check_vma=False)
```
